128 devices in a mesh: dp: 8 (over y, core), list: 16 (over x, z).
Axes of the slice: x: 4, y: 4, z: 4, core: 2. Of those that a mesh axis runs over, the one named last changes fastest.
Arguments:
- embeddings: bfloat16 [65536, 1024], P(('dp', 'list')), may hold values from -6 to 6
- coarse_id: int32 [65536], P(('dp', 'list')), may hold values from 0 to 8191, as said below
- fine_id: int32 [65536], P(('dp', 'list')), may hold values from 0 to 63
- list_home: int32 [8192], replicated, may hold values from 0 to 8191, as said below
- coarse_old: bfloat16 [8192, 1024], P('list'), may hold values from -6 to 6
Outputs:
- residual: bfloat16 [65536, 1024], P(('dp', 'list'))
- coarse_new: float32 [8192, 1024], P('list')
The draws below stay inside these ranges and needn't reach their ends.
Inputs may be any that keep to these rules, and one draw needn't show every extreme that they name: list_home is a permutation of 0 .. 8191. The device of a row is the one with dp index fine_id // 8 and list index list_home[coarse_id] // 512. Among the rows of one device at most 12 have the same device, and in every draw some device is the device of exactly 12 rows of every device.
All inputs are finite; a program needn't handle non-finite values.
Results may differ from the reference program's by a relative error of at most 0.0055.
Values may be sent and summed in bfloat16 or wider, within the bound.
No kernel may reach another device: no remote copies, remote signals or barrier semaphores. Data moves between devices by JAX's collectives and lax.ppermute only.
A program may use at most 128 MiB of HBM per device.

```python
import jax
import jax.numpy as jnp

D = 1024
LISTS_DEV = 512
FINE = 64
ROWS_DEV = 512
LISTS = 8192
ROWS = 65536
N_DP = 8
N_LIST = 16
DEVICES = 128


def layout(base):
    home = jax.random.permutation(jax.random.fold_in(base, 101), LISTS).astype(jnp.int32)
    inverse = jnp.zeros((LISTS,), jnp.int32).at[home].set(jnp.arange(LISTS, dtype=jnp.int32))
    peers = DEVICES
    share = ROWS_DEV // peers
    ranks = jnp.arange(peers, dtype=jnp.int32)
    quota = jnp.where(ranks == 0, 3 * share, jnp.where(ranks >= peers - 2, 0, share))
    bounds = jnp.cumsum(quota)
    rank_of = jnp.searchsorted(bounds, jnp.arange(ROWS_DEV, dtype=jnp.int32), side='right').astype(jnp.int32)
    hottest = jax.random.permutation(jax.random.fold_in(base, 102), peers).astype(jnp.int32)
    block_keys = jax.random.split(jax.random.fold_in(base, 103), peers)

    def one_block(block_key):
        first_key, second_key = jax.random.split(block_key)
        others = jax.random.permutation(first_key, peers - 1)
        order = jnp.concatenate([hottest[:1], hottest[1:][others]])
        shuffle = jax.random.permutation(second_key, ROWS_DEV)
        return order[rank_of[shuffle]]
    target = jax.vmap(one_block)(block_keys).reshape(-1)
    slot_keys = jax.random.split(jax.random.fold_in(base, 104), 4)
    count = ROWS_DEV * peers
    slot_one = jax.random.randint(slot_keys[0], (count,), 0, LISTS_DEV)
    slot_two = jax.random.randint(slot_keys[1], (count,), 0, LISTS_DEV)
    slot_three = jax.random.randint(slot_keys[2], (count,), 0, LISTS_DEV)
    slot = jnp.minimum(jnp.minimum(slot_one, slot_two), slot_three)
    inner = jax.random.randint(slot_keys[3], (count,), 0, FINE // N_DP)
    owner = target % N_LIST
    group = target // N_LIST
    coarse = inverse[owner * LISTS_DEV + slot].astype(jnp.int32)
    fine = (group * (FINE // N_DP) + inner).astype(jnp.int32)
    return (home, coarse, fine)


def draw_list_home(key, part):
    return layout(key)[0]


def draw_coarse_id(key, part):
    return layout(key)[1]


def draw_fine_id(key, part):
    return layout(key)[2]


def shard_levels(key, dims, shards, low, high):
    loudness, own = 1.0, jax.random.fold_in(key, 6)
    for dim, blocks in shards:
        heights = jnp.exp(jax.random.uniform(jax.random.fold_in(own, dim), (blocks,), jnp.float32, low / len(shards), high / len(shards)))
        loudness = loudness * jnp.repeat(heights, dims[dim] // blocks).reshape([-1 if axis == dim else 1 for axis in range(len(dims))])
    return loudness


def scatter_about(stream_key, dims, scale, limit, cuts=(), kind=jnp.bfloat16):
    array = jax.random.normal(stream_key, dims, jnp.float32) * scale
    if len(cuts) > 0:
        array = shard_levels(stream_key, dims, cuts, -0.22, 0.18) * array
    return jnp.clip(array, min=-limit, max=limit).astype(kind)


def setup_inputs(seed: int = 0) -> dict:
    seeds = jax.random.split(jax.random.key(seed), 6)
    embeddings = scatter_about(seeds[0], (ROWS, D), 1.0, 6.0, ((0, 128),))
    coarse_id = draw_coarse_id(jax.random.fold_in(seeds[5], 71), 0)
    fine_id = draw_fine_id(jax.random.fold_in(seeds[5], 71), 0)
    list_home = draw_list_home(jax.random.fold_in(seeds[5], 71), 0)
    coarse_old = scatter_about(seeds[4], (LISTS, D), 1.0, 6.0, ((0, 16),))
    return dict(embeddings=embeddings, coarse_id=coarse_id, fine_id=fine_id, list_home=list_home, coarse_old=coarse_old)


def reference(embeddings, coarse_id, fine_id, list_home, coarse_old):
    position = list_home[coarse_id].astype(jnp.int32)
    widened = embeddings.astype(jnp.float32)
    list_sum = jax.ops.segment_sum(widened, position, num_segments=LISTS)
    list_count = jax.ops.segment_sum(jnp.ones(position.shape, jnp.float32), position, num_segments=LISTS)
    coarse_new = (coarse_old.astype(jnp.float32) + list_sum) / (1.0 + list_count)[:, None]
    centered = widened - coarse_new[position]
    combined = position * FINE + fine_id
    unique_keys, inverse = jnp.unique(combined, size=combined.shape[0], return_inverse=True)
    inverse = inverse.reshape(-1).astype(jnp.int32)
    fine_sum = jax.ops.segment_sum(centered, inverse, num_segments=combined.shape[0])
    fine_count = jax.ops.segment_sum(jnp.ones(inverse.shape, jnp.float32), inverse, num_segments=combined.shape[0])
    fine_mean = fine_sum / (1.0 + fine_count)[:, None]
    residual = (centered - fine_mean[inverse]).astype(jnp.bfloat16)
    return residual, coarse_new
```

```python
import math

import jax
import jax.numpy as jnp
from jax import lax
from jax.experimental import pallas as pl
from jax.experimental.pallas import tpu as pltpu
from jax.sharding import PartitionSpec as P

FINE = 64
LANES = 128
KEY_ROWS = 8
VMEM_LIMIT = 62 * 1024 * 1024
WHOLE = pl.BlockSpec(memory_space=pltpu.VMEM)
SCALAR = pl.BlockSpec(memory_space=pltpu.SMEM)


def iota(shape, dim):
    return lax.broadcasted_iota(jnp.int32, shape, dim)


def ones_where(mask):
    return jnp.where(mask, 1.0, 0.0).astype(jnp.bfloat16)


def product(a, b, dims=((1,), (0,))):
    return lax.dot_general(a, b, (dims, ((), ())), preferred_element_type=jnp.float32)


def one_row(ref):
    return jnp.concatenate([ref[q : q + 1, :] for q in range(ref.shape[0])], axis=1)


def pack_kernel(cap, owners, slices, lists_here, me_ref, coarse_ref, fine_ref, home_ref, rows_ref, out_ref, placed_ref, keys_ref):
    rows = rows_ref.shape[0]
    block = cap + KEY_ROWS
    coarse, fine = one_row(coarse_ref), one_row(fine_ref)
    table_rows = home_ref.shape[0]
    home = home_ref[...]
    column = ones_where(iota((LANES, rows), 0) == (coarse & (LANES - 1)))
    high = product((home >> 7).astype(jnp.float32).astype(jnp.bfloat16), column)
    low = product((home & 127).astype(jnp.float32).astype(jnp.bfloat16), column)
    in_row = iota((table_rows, rows), 0) == (coarse >> 7)
    position = jnp.sum(jnp.where(in_row, high * 128.0 + low, 0.0), axis=0, keepdims=True).astype(jnp.int32)
    owner = position // lists_here
    slot = position - owner * lists_here
    key = slot * FINE + fine
    mine = iota((owners, rows), 0) == owner
    before = product(ones_where(mine), ones_where(iota((rows, rows), 0) < iota((rows, rows), 1)))
    rank = jnp.sum(jnp.where(mine, before, 0.0), axis=0, keepdims=True).astype(jnp.int32)
    fits = rank < cap
    over = jnp.max(jnp.where(fits, 0.0, 1.0))
    placed_ref[...] = jnp.where(fits, owner * cap + rank, -1)
    lane = (me_ref[0] * cap + rank) & (LANES - 1)
    spread = ones_where(iota((LANES, rows), 0) == jnp.where(fits, lane, -1))
    key_high = jnp.where(mine, ((key >> 8) + 1).astype(jnp.float32), 0.0).astype(jnp.bfloat16)
    key_low = jnp.where(mine, (key & 255).astype(jnp.float32), 0.0).astype(jnp.bfloat16)
    lanes_high = product(key_high, spread, ((1,), (1,)))
    lanes_low = product(key_low, spread, ((1,), (1,)))
    line = iota((KEY_ROWS, LANES), 0)
    keys_ref[...] = jnp.zeros_like(keys_ref)
    for o in range(owners):
        tile = jnp.where(line == 0, lanes_high[o : o + 1, :], jnp.where(line == 1, lanes_low[o : o + 1, :], 0.0))
        keys_ref[o * block + cap : (o + 1) * block, :] = jnp.where(line == 2, over, tile)
    where_to = jnp.where(fits, owner * block + rank, -1)
    place = ones_where(iota((owners * block, rows), 0) == where_to)
    for pair in range(slices // 2):
        both = product(place, rows_ref[:, pair * 2 * LANES : (pair + 1) * 2 * LANES])
        for half in range(2):
            piece = both[:, half * LANES : (half + 1) * LANES] + keys_ref[...]
            out_ref[2 * pair + half, :, :] = piece.astype(jnp.bfloat16)


def lists_kernel(cap, sources, lists_here, got_ref, old_ref, aug_ref, key_ref, split_ref, new_ref, over_ref, tile_ref, raw_ref, sums_ref):
    lane_rows = sources * cap // LANES
    for s in range(0, sources, 16):
        tile_ref[s * KEY_ROWS : (s + 16) * KEY_ROWS, :] = (
            got_ref[s : s + 16, cap : cap + KEY_ROWS, :].astype(jnp.float32).reshape(16 * KEY_ROWS, LANES)
        )
    high = tile_ref[pl.ds(0, sources, stride=KEY_ROWS), :]
    low = tile_ref[pl.ds(1, sources, stride=KEY_ROWS), :]
    over_ref[0, 0] = jnp.max(tile_ref[pl.ds(2, sources, stride=KEY_ROWS), :])
    raw_ref[...] = jnp.where(high > 0.0, (high - 1.0) * 256.0 + low, -1.0).astype(jnp.int32)
    period = LANES // math.gcd(cap, LANES)
    lines = period * cap // LANES
    groups = sources // period
    lane = iota((groups, LANES), 1)
    for r in range(lines):
        first, last = r * LANES // cap, (r * LANES + LANES - 1) // cap
        value = raw_ref[pl.ds(first, groups, stride=period), :]
        for a in range(first + 1, last + 1):
            value = jnp.where(lane >= a * cap - r * LANES, raw_ref[pl.ds(a, groups, stride=period), :], value)
        key_ref[pl.ds(r, groups, stride=lines), :] = value

    per = 2 * period
    chunk = period * cap

    def copy_rows(g, carry):
        base = pl.multiple_of(g * period, period)
        wide = got_ref[pl.ds(base, period), 0:cap, :].astype(jnp.float32).reshape(chunk, LANES)
        aug_ref[pl.ds(pl.multiple_of(g * chunk, LANES), chunk), 0:LANES] = wide.astype(jnp.bfloat16)
        aug_ref[pl.ds(pl.multiple_of(g * chunk, LANES), chunk), LANES : 2 * LANES] = jnp.ones((chunk, LANES), jnp.bfloat16)
        return carry

    lax.fori_loop(0, groups, copy_rows, 0)
    sums_ref[...] = jnp.zeros_like(sums_ref)
    step = 8
    lists = iota((lists_here, LANES), 0)

    def add(t, carry):
        base = t * step
        parts = [ones_where(lists == (key_ref[pl.ds(base + q, 1), :] >> 6)) for q in range(step)]
        chosen = jnp.concatenate(parts, axis=1)
        start = pl.multiple_of(base * LANES, step * LANES)
        sums_ref[...] += product(chosen, aug_ref[pl.ds(start, step * LANES), :])
        return carry

    lax.fori_loop(0, lane_rows // step, add, 0)
    new = (old_ref[...].astype(jnp.float32) + sums_ref[:, 0:LANES]) / (1.0 + sums_ref[:, LANES : 2 * LANES])
    rounded = new.astype(jnp.bfloat16)
    for d in range(new_ref.shape[0]):
        new_ref[d] = rounded
    split_ref[:, 0:LANES] = rounded
    split_ref[:, LANES : 2 * LANES] = (new - rounded.astype(jnp.float32)).astype(jnp.bfloat16)


def cells_kernel(cap, sources, lists_here, aug_ref, key_ref, split_ref, out_ref, turned_ref, total_ref):
    lane_rows = sources * cap // LANES
    high = 4
    step = 8
    block = high * LANES

    def rows_of(b, carry):
        start = pl.multiple_of(b * block, block)
        own = key_ref[pl.ds(b * high, high), :]
        square = jnp.concatenate([own, jnp.full((LANES - high, LANES), -2, jnp.int32)], axis=0)
        turned = square.astype(jnp.float32).T.astype(jnp.int32)
        columns = [jnp.broadcast_to(turned[:, q : q + 1], (LANES, LANES)) for q in range(high)]
        for q in range(high):
            turned_ref[q * LANES : (q + 1) * LANES, :] = columns[q]
        def part_sum(base, count):
            left = turned_ref[...]
            parts = [ones_where(left == key_ref[pl.ds(base + q, 1), :]) for q in range(count)]
            at = base * LANES if isinstance(base, int) else pl.multiple_of(base * LANES, LANES)
            return product(jnp.concatenate(parts, axis=1), aug_ref[pl.ds(at, count * LANES), :])

        if lane_rows <= 48:
            total_ref[...] = sum(part_sum(t, step) for t in range(0, lane_rows, step))
        else:
            total_ref[...] = jnp.zeros_like(total_ref)

            def add(t, inner):
                total_ref[...] += part_sum(t * step, step)
                return inner

            lax.fori_loop(0, lane_rows // step, add, 0)
        slots = turned_ref[...] >> 6
        parts = [ones_where(slots == iota((block, LANES), 1) + q * LANES) for q in range(lists_here // LANES)]
        centre = product(jnp.concatenate(parts, axis=1), split_ref[...])
        own_rows = aug_ref[pl.ds(start, block), 0:LANES].astype(jnp.float32)
        mean = (centre[:, 0:LANES] + centre[:, LANES : 2 * LANES] + total_ref[:, 0:LANES]) / (
            1.0 + total_ref[:, LANES : 2 * LANES]
        )
        out_ref[pl.ds(start, block), :] = (own_rows - mean).astype(jnp.bfloat16)
        return carry

    lax.fori_loop(0, lane_rows // high, rows_of, 0)


def unpack_kernel(cap, owners, slices, placed_ref, back_ref, parts_ref, out_ref, new_ref):
    rows = out_ref.shape[0]
    placed = placed_ref[...].astype(jnp.float32)
    lines = [placed[:, q * LANES : (q + 1) * LANES] for q in range(rows // LANES)]
    column = jnp.concatenate([jnp.broadcast_to(line, (LANES, LANES)).T for line in lines], axis=0).astype(jnp.int32)
    parts = [ones_where(column == iota((rows, LANES), 1) + r * LANES) for r in range(owners * cap // LANES)]
    take = jnp.concatenate(parts, axis=1)
    for d in range(0, slices, 2):
        both = jnp.concatenate([back_ref[d], back_ref[d + 1]], axis=1)
        out_ref[:, d * LANES : (d + 2) * LANES] = product(take, both).astype(jnp.bfloat16)
    for d in range(slices):
        new_ref[:, d * LANES : (d + 1) * LANES] = parts_ref[d].astype(jnp.float32)


def call(kernel, outs, scratch, in_specs, out_specs, flops, name):
    return pl.pallas_call(
        kernel,
        out_shape=outs,
        in_specs=in_specs,
        out_specs=out_specs,
        scratch_shapes=scratch,
        compiler_params=pltpu.CompilerParams(vmem_limit_bytes=VMEM_LIMIT),
        cost_estimate=pl.CostEstimate(flops=flops, bytes_accessed=4 << 20, transcendentals=0),
        name=name,
    )


def iterate(cap, me, mine, coarse, fine, home, embeddings, coarse_old):
    slices, owners = lax.axis_size("dp"), lax.axis_size("list")
    peers = slices * owners
    rows, width = embeddings.shape
    lists_here = coarse_old.shape[0]
    block = cap + KEY_ROWS
    total = peers * cap
    shape = jax.ShapeDtypeStruct
    from functools import partial

    packed, placed = call(
        partial(pack_kernel, cap, owners, slices, lists_here),
        (shape((slices, owners * block, LANES), jnp.bfloat16), shape((1, rows), jnp.int32)),
        [pltpu.VMEM((owners * block, LANES), jnp.float32)],
        [SCALAR, WHOLE, WHOLE, WHOLE, WHOLE],
        (WHOLE, WHOLE),
        4 * rows * owners * block * width,
        "pack",
    )(me, coarse, fine, home, embeddings)
    got = lax.all_to_all(packed.reshape(peers, block, LANES), ("dp", "list"), 0, 0, tiled=True)
    old_part = lax.dynamic_slice_in_dim(coarse_old, mine * LANES, LANES, 1)
    aug, keys, split, new_part, over = call(
        partial(lists_kernel, cap, peers, lists_here),
        (
            shape((total, 2 * LANES), jnp.bfloat16),
            shape((total // LANES, LANES), jnp.int32),
            shape((lists_here, 2 * LANES), jnp.bfloat16),
            shape((slices, lists_here, LANES), jnp.bfloat16),
            shape((1, 1), jnp.float32),
        ),
        [
            pltpu.VMEM((peers * KEY_ROWS, LANES), jnp.float32),
            pltpu.VMEM((peers, LANES), jnp.int32),
            pltpu.VMEM((lists_here, 2 * LANES), jnp.float32),
        ],
        [WHOLE, WHOLE],
        (WHOLE, WHOLE, WHOLE, WHOLE, SCALAR),
        4 * total * lists_here * LANES,
        "lists",
    )(got, old_part)
    new_parts = lax.all_to_all(new_part, "dp", 0, 0, tiled=True)
    done = call(
        partial(cells_kernel, cap, peers, lists_here),
        shape((total, LANES), jnp.bfloat16),
        [pltpu.VMEM((4 * LANES, LANES), jnp.int32), pltpu.VMEM((4 * LANES, 2 * LANES), jnp.float32)],
        [WHOLE, WHOLE, WHOLE],
        WHOLE,
        4 * total * total * LANES,
        "cells",
    )(aug, keys, split)
    back = lax.all_to_all(done.reshape(peers, cap, LANES), ("dp", "list"), 0, 0, tiled=True)

    def finish(placed, back, new_parts):
        return call(
            partial(unpack_kernel, cap, owners, slices),
            (shape((rows, width), jnp.bfloat16), shape((lists_here, width), jnp.float32)),
            [],
            [WHOLE, WHOLE, WHOLE],
            (WHOLE, WHOLE),
            2 * rows * owners * cap * width,
            "unpack",
        )(placed, back.reshape(slices, owners * cap, LANES), new_parts)

    return over, finish, (placed, back, new_parts)


def on_device(embeddings, coarse_id, fine_id, list_home, coarse_old):
    mine = lax.axis_index("dp")
    me = (mine * lax.axis_size("list") + lax.axis_index("list")).reshape(1)
    rows = embeddings.shape[0]
    args = (
        me,
        mine,
        coarse_id.reshape(rows // LANES, LANES),
        fine_id.reshape(rows // LANES, LANES),
        list_home.reshape(-1, LANES),
        embeddings,
        coarse_old,
    )
    capacity, bound = 40, 96
    over, finish, parts = iterate(capacity, *args)

    def again(parts, args):
        _, finish_all, parts_all = iterate(bound, *args)
        return finish_all(*parts_all)

    return lax.cond(over[0, 0] > 0.0, again, lambda parts, args: finish(*parts), parts, args)


def solution(mesh):
    return jax.shard_map(
        on_device,
        mesh=mesh,
        in_specs=(
            P(("dp", "list"), None),
            P(("dp", "list")),
            P(("dp", "list")),
            P(),
            P("list", None),
        ),
        out_specs=(P(("dp", "list"), None), P("list", None)),
        check_vma=False,
    )
```

```python
from functools import partial

import jax
import jax.numpy as jnp
from jax import lax
from jax.experimental import pallas as pl
from jax.experimental.pallas import tpu as pltpu
from jax.sharding import PartitionSpec as P

FINE = 64
LANES = 128
KEY_ROWS = 8
HIGH = 4
MIB = 1024 * 1024
WHOLE = pl.BlockSpec(memory_space=pltpu.VMEM)
SCALAR = pl.BlockSpec(memory_space=pltpu.SMEM)


def iota(shape, dim):
    return lax.broadcasted_iota(jnp.int32, shape, dim)


def ones_where(mask):
    return jnp.where(mask, 1.0, 0.0).astype(jnp.bfloat16)


def product(a, b, dims=((1,), (0,))):
    return lax.dot_general(a, b, (dims, ((), ())), preferred_element_type=jnp.float32)


def one_row(ref):
    return jnp.concatenate([ref[q : q + 1, :] for q in range(ref.shape[0])], axis=1)


def pack_kernel(cap, owners, slices, lists_here, coarse_ref, fine_ref, home_ref, rows_ref, out_ref, placed_ref, keys_ref):
    rows = rows_ref.shape[0]
    block = cap + KEY_ROWS
    peers = owners * slices
    coarse, fine = one_row(coarse_ref), one_row(fine_ref)
    table_rows = home_ref.shape[0]
    home = home_ref[...]
    column = ones_where(iota((LANES, rows), 0) == (coarse & (LANES - 1)))
    high = product((home >> 7).astype(jnp.float32).astype(jnp.bfloat16), column)
    low = product((home & 127).astype(jnp.float32).astype(jnp.bfloat16), column)
    in_row = iota((table_rows, rows), 0) == (coarse >> 7)
    position = jnp.sum(jnp.where(in_row, high * 128.0 + low, 0.0), axis=0, keepdims=True).astype(jnp.int32)
    owner = position // lists_here
    slot = position - owner * lists_here
    key = slot * FINE + fine
    target = ones_where(iota((peers, rows), 0) == owner * slices + fine // (FINE // slices))
    before = product(target, ones_where(iota((rows, rows), 0) < iota((rows, rows), 1)))
    counts = product(target, jnp.ones((rows, LANES), jnp.bfloat16))
    line, other = iota((peers, peers), 0), iota((peers, peers), 1)
    lower = ones_where((other < line) & (other // slices == line // slices))
    base = product(lower, counts.astype(jnp.bfloat16))
    base = jnp.concatenate([base] * (rows // LANES), axis=1)
    picked = jnp.where(target.astype(jnp.float32) > 0.0, before + base, 0.0)
    rank = jnp.sum(picked, axis=0, keepdims=True).astype(jnp.int32)
    fits = rank < cap
    over = jnp.max(jnp.where(fits, 0.0, 1.0))
    placed_ref[...] = jnp.where(fits, owner * cap + rank, -1)
    mine = iota((owners, rows), 0) == owner
    spread = ones_where(iota((LANES, rows), 0) == jnp.where(fits, rank, -1))
    key_high = jnp.where(mine, ((key >> 8) + 1).astype(jnp.float32), 0.0).astype(jnp.bfloat16)
    key_low = jnp.where(mine, (key & 255).astype(jnp.float32), 0.0).astype(jnp.bfloat16)
    lanes_high = product(key_high, spread, ((1,), (1,)))
    lanes_low = product(key_low, spread, ((1,), (1,)))
    line = iota((KEY_ROWS, LANES), 0)
    keys_ref[...] = jnp.zeros_like(keys_ref)
    for o in range(owners):
        tile = jnp.where(line == 0, lanes_high[o : o + 1, :], jnp.where(line == 1, lanes_low[o : o + 1, :], 0.0))
        keys_ref[o * block + cap : (o + 1) * block, :] = jnp.where(line == 2, over, tile)
    where_to = jnp.where(fits, owner * block + rank, -1)
    place = ones_where(iota((owners * block, rows), 0) == where_to)
    for pair in range(slices // 2):
        both = product(place, rows_ref[:, pair * 2 * LANES : (pair + 1) * 2 * LANES])
        for half in range(2):
            piece = both[:, half * LANES : (half + 1) * LANES] + keys_ref[...]
            out_ref[2 * pair + half, :, :] = piece.astype(jnp.bfloat16)


def lists_kernel(cap, sources, lists_here, fine_here, got_ref, old_ref, aug_ref, key_ref, span_ref, split_ref, new_ref, over_ref, tile_ref):
    for s in range(0, sources, 16):
        tile_ref[s * KEY_ROWS : (s + 16) * KEY_ROWS, :] = (
            got_ref[s : s + 16, cap : cap + KEY_ROWS, :].astype(jnp.float32).reshape(16 * KEY_ROWS, LANES)
        )
    high = tile_ref[pl.ds(0, sources, stride=KEY_ROWS), :]
    low = tile_ref[pl.ds(1, sources, stride=KEY_ROWS), :]
    over_ref[0, 0] = jnp.max(tile_ref[pl.ds(2, sources, stride=KEY_ROWS), :])
    raw = jnp.where(high > 0.0, (high - 1.0) * 256.0 + low, -1.0)
    key_ref[...] = raw.T.astype(jnp.int32)

    keys = raw.astype(jnp.int32)
    group = (keys & (FINE - 1)) // fine_here
    least = jnp.min(jnp.where(keys >= 0, group, FINE), axis=0, keepdims=True)
    most = jnp.max(jnp.where(keys >= 0, group, -1), axis=0, keepdims=True)
    blocks = span_ref.shape[0]
    lane = iota((blocks, LANES), 1)
    inside = lane // HIGH == iota((blocks, LANES), 0)
    first = jnp.min(jnp.where(inside, least, FINE), axis=1, keepdims=True)
    last = jnp.max(jnp.where(inside, most, -1), axis=1, keepdims=True)
    meet = (most >= first) & (least <= last)
    start = jnp.min(jnp.where(meet, lane, LANES), axis=1, keepdims=True)
    stop = jnp.max(jnp.where(meet, lane + 1, 0), axis=1, keepdims=True)
    span_ref[...] = jnp.where(lane == 0, start, stop)

    part = 16
    for s in range(0, sources, part):
        wide = got_ref[s : s + part, 0:cap, :].astype(jnp.float32)
        aug_ref[:, s : s + part, 0:LANES] = jnp.transpose(wide, (1, 0, 2)).astype(jnp.bfloat16)
    aug_ref[:, :, LANES : 2 * LANES] = jnp.ones((cap, sources, LANES), jnp.bfloat16)
    step = 8
    lists = iota((lists_here, LANES), 0)

    def part_sum(base):
        parts = [ones_where(lists == (key_ref[base + q : base + q + 1, :] >> 6)) for q in range(step)]
        return product(jnp.concatenate(parts, axis=1), aug_ref[base : base + step].reshape(step * sources, 2 * LANES))

    sums = sum(part_sum(t) for t in range(0, cap, step))
    new = (old_ref[...].astype(jnp.float32) + sums[:, 0:LANES]) / (1.0 + sums[:, LANES : 2 * LANES])
    rounded = new.astype(jnp.bfloat16)
    for d in range(new_ref.shape[0]):
        new_ref[d] = rounded
    split_ref[:, 0:LANES] = rounded
    split_ref[:, LANES : 2 * LANES] = (new - rounded.astype(jnp.float32)).astype(jnp.bfloat16)


def cells_kernel(cap, sources, lists_here, aug_ref, key_ref, span_ref, split_ref, out_ref, total_ref, done_ref):
    step = 16 if cap > 16 else cap
    block = HIGH * sources

    def rows_of(b, carry):
        first, stop = span_ref[b, 0], span_ref[b, 1]
        start = pl.multiple_of(b * block, block)

        @pl.when(first >= stop)
        def _():
            done_ref[pl.ds(start, block), :] = jnp.zeros((block, LANES), jnp.float32)

        @pl.when(first < stop)
        def _():
            own = key_ref[pl.ds(b * HIGH, HIGH), :]
            square = jnp.concatenate([own, jnp.full((LANES - HIGH, LANES), -2, jnp.int32)], axis=0)
            turned = square.astype(jnp.float32).T.astype(jnp.int32)
            left = jnp.concatenate(
                [jnp.broadcast_to(turned[:, q : q + 1], (LANES, LANES)) for q in range(HIGH)], axis=0
            )

            def part_sum(t):
                wanted = first + t * step
                base = jnp.minimum(wanted, cap - step)
                parts = []
                for q in range(step):
                    row = key_ref[pl.ds(base + q, 1), :]
                    parts.append(ones_where(left == jnp.where(base + q >= wanted, row, -3)))
                right = aug_ref[pl.ds(base, step)].reshape(step * sources, 2 * LANES)
                return product(jnp.concatenate(parts, axis=1), right)

            slots = left >> 6
            parts = [ones_where(slots == iota((block, LANES), 1) + q * LANES) for q in range(lists_here // LANES)]
            centre = product(jnp.concatenate(parts, axis=1), split_ref[...])
            centre = centre[:, 0:LANES] + centre[:, LANES : 2 * LANES]
            total = part_sum(0)
            total_ref[:, 0:LANES] = total[:, 0:LANES] + centre
            total_ref[:, LANES : 2 * LANES] = total[:, LANES : 2 * LANES] + 1.0

            def more(t, inner):
                total_ref[...] += part_sum(t)
                return inner

            lax.fori_loop(1, (stop - first + step - 1) // step, more, 0)
            own_rows = aug_ref[pl.ds(b * HIGH, HIGH), :, 0:LANES].astype(jnp.float32).reshape(block, LANES)
            mean = total_ref[:, 0:LANES] / total_ref[:, LANES : 2 * LANES]
            done_ref[pl.ds(start, block), :] = own_rows - mean

        return carry

    lax.fori_loop(0, cap // HIGH, rows_of, 0)
    part = 16
    for s in range(0, sources, part):
        piece = jnp.concatenate(
            [done_ref[k * sources + s : k * sources + s + part, :].reshape(1, part, LANES) for k in range(cap)], axis=0
        )
        out_ref[s : s + part] = jnp.transpose(piece, (1, 0, 2)).astype(jnp.bfloat16)


def unpack_kernel(cap, owners, slices, placed_ref, back_ref, parts_ref, out_ref, new_ref):
    rows = out_ref.shape[0]
    placed = placed_ref[...].astype(jnp.float32)
    lines = [placed[:, q * LANES : (q + 1) * LANES] for q in range(rows // LANES)]
    column = jnp.concatenate([jnp.broadcast_to(line, (LANES, LANES)).T for line in lines], axis=0).astype(jnp.int32)
    parts = [ones_where(column == iota((rows, LANES), 1) + r * LANES) for r in range(owners * cap // LANES)]
    take = jnp.concatenate(parts, axis=1)
    for d in range(0, slices, 2):
        both = jnp.concatenate([back_ref[d], back_ref[d + 1]], axis=1)
        out_ref[:, d * LANES : (d + 2) * LANES] = product(take, both).astype(jnp.bfloat16)
    for d in range(slices):
        new_ref[:, d * LANES : (d + 1) * LANES] = parts_ref[d].astype(jnp.float32)


def call(kernel, outs, scratch, in_specs, out_specs, flops, name, mib):
    return pl.pallas_call(
        kernel,
        out_shape=outs,
        in_specs=in_specs,
        out_specs=out_specs,
        scratch_shapes=scratch,
        compiler_params=pltpu.CompilerParams(vmem_limit_bytes=mib * MIB),
        cost_estimate=pl.CostEstimate(flops=flops, bytes_accessed=4 * MIB, transcendentals=0),
        name=name,
    )


def iterate(cap, mine, coarse, fine, home, embeddings, coarse_old):
    slices, owners = lax.axis_size("dp"), lax.axis_size("list")
    peers = slices * owners
    rows, width = embeddings.shape
    lists_here = coarse_old.shape[0]
    block = cap + KEY_ROWS
    total = peers * cap
    mib = 16 if cap <= 48 else 40
    shape = jax.ShapeDtypeStruct

    packed, placed = call(
        partial(pack_kernel, cap, owners, slices, lists_here),
        (shape((slices, owners * block, LANES), jnp.bfloat16), shape((1, rows), jnp.int32)),
        [pltpu.VMEM((owners * block, LANES), jnp.float32)],
        [WHOLE, WHOLE, WHOLE, WHOLE],
        (WHOLE, WHOLE),
        4 * rows * owners * block * width,
        "pack",
        mib,
    )(coarse, fine, home, embeddings)
    got = lax.all_to_all(packed.reshape(peers, block, LANES), ("dp", "list"), 0, 0, tiled=True)
    old_part = lax.dynamic_slice_in_dim(coarse_old, mine * LANES, LANES, 1)
    aug, keys, span, split, new_part, over = call(
        partial(lists_kernel, cap, peers, lists_here, FINE // slices),
        (
            shape((cap, peers, 2 * LANES), jnp.bfloat16),
            shape((LANES, peers), jnp.int32),
            shape((-(-cap // (8 * HIGH)) * 8, LANES), jnp.int32),
            shape((lists_here, 2 * LANES), jnp.bfloat16),
            shape((slices, lists_here, LANES), jnp.bfloat16),
            shape((1, 1), jnp.float32),
        ),
        [pltpu.VMEM((peers * KEY_ROWS, LANES), jnp.float32)],
        [WHOLE, WHOLE],
        (WHOLE, WHOLE, WHOLE, WHOLE, WHOLE, SCALAR),
        4 * total * lists_here * LANES,
        "lists",
        mib,
    )(got, old_part)
    new_parts = lax.all_to_all(new_part, "dp", 0, 0, tiled=True)
    done = call(
        partial(cells_kernel, cap, peers, lists_here),
        shape((peers, cap, LANES), jnp.bfloat16),
        [pltpu.VMEM((HIGH * LANES, 2 * LANES), jnp.float32), pltpu.VMEM((total, LANES), jnp.float32)],
        [WHOLE, WHOLE, SCALAR, WHOLE],
        WHOLE,
        4 * total * total * LANES,
        "cells",
        mib,
    )(aug, keys, span, split)
    back = lax.all_to_all(done, ("dp", "list"), 0, 0, tiled=True)

    def finish(placed, back, new_parts):
        return call(
            partial(unpack_kernel, cap, owners, slices),
            (shape((rows, width), jnp.bfloat16), shape((lists_here, width), jnp.float32)),
            [],
            [WHOLE, WHOLE, WHOLE],
            (WHOLE, WHOLE),
            2 * rows * owners * cap * width,
            "unpack",
            mib,
        )(placed, back.reshape(slices, owners * cap, LANES), new_parts)

    return over, finish, (placed, back, new_parts)


def on_device(embeddings, coarse_id, fine_id, list_home, coarse_old):
    rows = embeddings.shape[0]
    args = (
        lax.axis_index("dp"),
        coarse_id.reshape(rows // LANES, LANES),
        fine_id.reshape(rows // LANES, LANES),
        list_home.reshape(-1, LANES),
        embeddings,
        coarse_old,
    )
    capacity, bound = 40, 96
    over, finish, parts = iterate(capacity, *args)

    def again(parts, args):
        _, finish_all, parts_all = iterate(bound, *args)
        return finish_all(*parts_all)

    return lax.cond(over[0, 0] > 0.0, again, lambda parts, args: finish(*parts), parts, args)


def solution(mesh):
    return jax.shard_map(
        on_device,
        mesh=mesh,
        in_specs=(
            P(("dp", "list"), None),
            P(("dp", "list")),
            P(("dp", "list")),
            P(),
            P("list", None),
        ),
        out_specs=(P(("dp", "list"), None), P("list", None)),
        check_vma=False,
    )
```

```python
from functools import partial

import jax
import jax.numpy as jnp
from jax import lax
from jax.experimental import pallas as pl
from jax.experimental.pallas import tpu as pltpu
from jax.sharding import PartitionSpec as P

FINE = 64
LANES = 128
KEY_ROWS = 8
HIGH = 4
STEP = 16
MIB = 1024 * 1024
WHOLE = pl.BlockSpec(memory_space=pltpu.VMEM)
SCALAR = pl.BlockSpec(memory_space=pltpu.SMEM)


def iota(shape, dim):
    return lax.broadcasted_iota(jnp.int32, shape, dim)


def ones_where(mask):
    return jnp.where(mask, 1.0, 0.0).astype(jnp.bfloat16)


def product(a, b, dims=((1,), (0,))):
    return lax.dot_general(a, b, (dims, ((), ())), preferred_element_type=jnp.float32)


def one_row(ref):
    return jnp.concatenate([ref[q : q + 1, :] for q in range(ref.shape[0])], axis=1)


def pack_kernel(cap, owners, slices, lists_here, coarse_ref, fine_ref, home_ref, rows_ref, out_ref, placed_ref, keys_ref):
    rows = rows_ref.shape[0]
    block = cap + KEY_ROWS
    peers = owners * slices
    coarse, fine = one_row(coarse_ref), one_row(fine_ref)
    table_rows = home_ref.shape[0]
    home = home_ref[...]
    column = ones_where(iota((LANES, rows), 0) == (coarse & (LANES - 1)))
    high = product((home >> 7).astype(jnp.float32).astype(jnp.bfloat16), column)
    low = product((home & 127).astype(jnp.float32).astype(jnp.bfloat16), column)
    in_row = iota((table_rows, rows), 0) == (coarse >> 7)
    position = jnp.sum(jnp.where(in_row, high * 128.0 + low, 0.0), axis=0, keepdims=True).astype(jnp.int32)
    owner = position // lists_here
    slot = position - owner * lists_here
    key = slot * FINE + fine
    target = ones_where(iota((peers, rows), 0) == owner * slices + fine // (FINE // slices))
    before = product(target, ones_where(iota((rows, rows), 0) < iota((rows, rows), 1)))
    counts = product(target, jnp.ones((rows, LANES), jnp.bfloat16))
    line, other = iota((peers, peers), 0), iota((peers, peers), 1)
    lower = ones_where((other < line) & (other // slices == line // slices))
    base = product(lower, counts.astype(jnp.bfloat16))
    base = jnp.concatenate([base] * (rows // LANES), axis=1)
    picked = jnp.where(target.astype(jnp.float32) > 0.0, before + base, 0.0)
    rank = jnp.sum(picked, axis=0, keepdims=True).astype(jnp.int32)
    fits = rank < cap
    over = jnp.max(jnp.where(fits, 0.0, 1.0))
    placed_ref[...] = jnp.where(fits, owner * cap + rank, -1)
    mine = iota((owners, rows), 0) == owner
    spread = ones_where(iota((LANES, rows), 0) == jnp.where(fits, rank, -1))
    key_high = jnp.where(mine, ((key >> 8) + 1).astype(jnp.float32), 0.0).astype(jnp.bfloat16)
    key_low = jnp.where(mine, (key & 255).astype(jnp.float32), 0.0).astype(jnp.bfloat16)
    lanes_high = product(key_high, spread, ((1,), (1,)))
    lanes_low = product(key_low, spread, ((1,), (1,)))
    line = iota((KEY_ROWS, LANES), 0)
    keys_ref[...] = jnp.zeros_like(keys_ref)
    for o in range(owners):
        tile = jnp.where(line == 0, lanes_high[o : o + 1, :], jnp.where(line == 1, lanes_low[o : o + 1, :], 0.0))
        keys_ref[o * block + cap : (o + 1) * block, :] = jnp.where(line == 2, over, tile)
    where_to = jnp.where(fits, owner * block + rank, -1)
    place = ones_where(iota((owners * block, rows), 0) == where_to)
    for pair in range(slices // 2):
        both = product(place, rows_ref[:, pair * 2 * LANES : (pair + 1) * 2 * LANES])
        for half in range(2):
            piece = both[:, half * LANES : (half + 1) * LANES] + keys_ref[...]
            out_ref[2 * pair + half, :, :] = piece.astype(jnp.bfloat16)


def middle_kernel(
    cap,
    sources,
    lists_here,
    fine_here,
    got_ref,
    old_ref,
    out_ref,
    new_ref,
    over_ref,
    aug_ref,
    key_ref,
    span_ref,
    near_ref,
    split_ref,
    total_ref,
    done_ref,
    tile_ref,
    copy_sem,
):
    for s in range(0, sources, 16):
        tile_ref[s * KEY_ROWS : (s + 16) * KEY_ROWS, :] = (
            got_ref[s : s + 16, cap : cap + KEY_ROWS, :].astype(jnp.float32).reshape(16 * KEY_ROWS, LANES)
        )
    high = tile_ref[pl.ds(0, sources, stride=KEY_ROWS), :]
    low = tile_ref[pl.ds(1, sources, stride=KEY_ROWS), :]
    over_ref[0, 0] = jnp.max(tile_ref[pl.ds(2, sources, stride=KEY_ROWS), :])
    raw = jnp.where(high > 0.0, (high - 1.0) * 256.0 + low, -1.0)
    key_ref[...] = raw.T.astype(jnp.int32)

    keys = raw.astype(jnp.int32)
    group = (keys & (FINE - 1)) // fine_here
    least = jnp.min(jnp.where(keys >= 0, group, FINE), axis=0, keepdims=True)
    most = jnp.max(jnp.where(keys >= 0, group, -1), axis=0, keepdims=True)
    blocks = span_ref.shape[0]
    lane = iota((blocks, LANES), 1)
    inside = lane // HIGH == iota((blocks, LANES), 0)
    first = jnp.min(jnp.where(inside, least, FINE), axis=1, keepdims=True)
    last = jnp.max(jnp.where(inside, most, -1), axis=1, keepdims=True)
    meet = (most >= first) & (least <= last)
    start = jnp.min(jnp.where(meet, lane, LANES), axis=1, keepdims=True)
    stop = jnp.max(jnp.where(meet, lane + 1, 0), axis=1, keepdims=True)
    span_ref[...] = jnp.where(lane == 0, start, stop)
    copy = pltpu.make_async_copy(span_ref, near_ref, copy_sem)
    copy.start()

    part = 16
    for s in range(0, sources, part):
        wide = got_ref[s : s + part, 0:cap, :].astype(jnp.float32)
        aug_ref[:, s : s + part, 0:LANES] = jnp.transpose(wide, (1, 0, 2)).astype(jnp.bfloat16)
    aug_ref[:, :, LANES : 2 * LANES] = jnp.ones((cap, sources, LANES), jnp.bfloat16)
    lists = iota((lists_here, LANES), 0)

    def list_sum(base):
        parts = [ones_where(lists == (key_ref[base + q : base + q + 1, :] >> 6)) for q in range(8)]
        return product(jnp.concatenate(parts, axis=1), aug_ref[base : base + 8].reshape(8 * sources, 2 * LANES))

    sums = sum(list_sum(t) for t in range(0, cap, 8))
    new = (old_ref[...].astype(jnp.float32) + sums[:, 0:LANES]) / (1.0 + sums[:, LANES : 2 * LANES])
    rounded = new.astype(jnp.bfloat16)
    new_ref[...] = rounded
    split_ref[:, 0:LANES] = rounded
    split_ref[:, LANES : 2 * LANES] = (new - rounded.astype(jnp.float32)).astype(jnp.bfloat16)
    copy.wait()

    step = STEP if cap > STEP else cap
    block = HIGH * sources

    def rows_of(b, carry):
        first, stop = near_ref[b, 0], near_ref[b, 1]
        start = pl.multiple_of(b * block, block)

        @pl.when(first >= stop)
        def _():
            done_ref[pl.ds(start, block), :] = jnp.zeros((block, LANES), jnp.float32)

        @pl.when(first < stop)
        def _():
            own = key_ref[pl.ds(b * HIGH, HIGH), :]
            square = jnp.concatenate([own, jnp.full((LANES - HIGH, LANES), -2, jnp.int32)], axis=0)
            turned = square.astype(jnp.float32).T.astype(jnp.int32)
            left = jnp.concatenate(
                [jnp.broadcast_to(turned[:, q : q + 1], (LANES, LANES)) for q in range(HIGH)], axis=0
            )
            narrow = left.astype(jnp.int16).reshape(block // 16, 16, LANES)

            def part_sum(t):
                wanted = first + t * step
                base = jnp.minimum(wanted, cap - step)
                parts = []
                for q in range(step):
                    row = jnp.where(base + q >= wanted, key_ref[pl.ds(base + q, 1), :], -3)
                    row = jnp.broadcast_to(row, (16, LANES)).astype(jnp.int16).reshape(1, 16, LANES)
                    same = jnp.where(narrow == row, jnp.bfloat16(1), jnp.bfloat16(0))
                    parts.append(same.reshape(block, LANES))
                right = aug_ref[pl.ds(base, step)].reshape(step * sources, 2 * LANES)
                return product(jnp.concatenate(parts, axis=1), right)

            slots = left >> 6
            parts = [ones_where(slots == iota((block, LANES), 1) + q * LANES) for q in range(lists_here // LANES)]
            centre = product(jnp.concatenate(parts, axis=1), split_ref[...])
            centre = centre[:, 0:LANES] + centre[:, LANES : 2 * LANES]
            total = part_sum(0)
            total_ref[:, 0:LANES] = total[:, 0:LANES] + centre
            total_ref[:, LANES : 2 * LANES] = total[:, LANES : 2 * LANES] + 1.0

            def more(t, inner):
                total_ref[...] += part_sum(t)
                return inner

            lax.fori_loop(1, (stop - first + step - 1) // step, more, 0)
            own_rows = aug_ref[pl.ds(b * HIGH, HIGH), :, 0:LANES].astype(jnp.float32).reshape(block, LANES)
            mean = total_ref[:, 0:LANES] / total_ref[:, LANES : 2 * LANES]
            done_ref[pl.ds(start, block), :] = own_rows - mean

        return carry

    lax.fori_loop(0, cap // HIGH, rows_of, 0)
    for s in range(0, sources, part):
        piece = jnp.concatenate(
            [done_ref[k * sources + s : k * sources + s + part, :].reshape(1, part, LANES) for k in range(cap)], axis=0
        )
        out_ref[s : s + part] = jnp.transpose(piece, (1, 0, 2)).astype(jnp.bfloat16)


def unpack_kernel(cap, owners, slices, mine_ref, placed_ref, back_ref, *refs):
    part_refs, (out_ref, new_ref) = refs[:-2], refs[-2:]
    rows = out_ref.shape[0]
    placed = placed_ref[...].astype(jnp.float32)
    lines = [placed[:, q * LANES : (q + 1) * LANES] for q in range(rows // LANES)]
    column = jnp.concatenate([jnp.broadcast_to(line, (LANES, LANES)).T for line in lines], axis=0).astype(jnp.int32)
    parts = [ones_where(column == iota((rows, LANES), 1) + r * LANES) for r in range(owners * cap // LANES)]
    take = jnp.concatenate(parts, axis=1)
    for d in range(0, slices, 2):
        both = jnp.concatenate([back_ref[d], back_ref[d + 1]], axis=1)
        out_ref[:, d * LANES : (d + 2) * LANES] = product(take, both).astype(jnp.bfloat16)
    for k, part_ref in enumerate(part_refs):
        at = pl.multiple_of((mine_ref[0] ^ k) * LANES, LANES)
        new_ref[:, pl.ds(at, LANES)] = part_ref[...].astype(jnp.float32)


def call(kernel, outs, scratch, in_specs, out_specs, flops, name, mib):
    return pl.pallas_call(
        kernel,
        out_shape=outs,
        in_specs=in_specs,
        out_specs=out_specs,
        scratch_shapes=scratch,
        compiler_params=pltpu.CompilerParams(vmem_limit_bytes=mib * MIB),
        cost_estimate=pl.CostEstimate(flops=flops, bytes_accessed=4 * MIB, transcendentals=0),
        name=name,
    )


def middle_scratch(cap, peers, lists_here):
    blocks = -(-cap // (8 * HIGH)) * 8
    return [
        pltpu.VMEM((cap, peers, 2 * LANES), jnp.bfloat16),
        pltpu.VMEM((LANES, peers), jnp.int32),
        pltpu.VMEM((blocks, LANES), jnp.int32),
        pltpu.SMEM((blocks, LANES), jnp.int32),
        pltpu.VMEM((lists_here, 2 * LANES), jnp.bfloat16),
        pltpu.VMEM((HIGH * LANES, 2 * LANES), jnp.float32),
        pltpu.VMEM((peers * cap, LANES), jnp.float32),
        pltpu.VMEM((peers * KEY_ROWS, LANES), jnp.float32),
        pltpu.SemaphoreType.DMA,
    ]


def iterate(cap, mine, coarse, fine, home, embeddings, coarse_old):
    slices, owners = lax.axis_size("dp"), lax.axis_size("list")
    peers = slices * owners
    rows, width = embeddings.shape
    lists_here = coarse_old.shape[0]
    block = cap + KEY_ROWS
    total = peers * cap
    mib = 20 if cap <= 48 else 40
    shape = jax.ShapeDtypeStruct

    packed, placed = call(
        partial(pack_kernel, cap, owners, slices, lists_here),
        (shape((slices, owners * block, LANES), jnp.bfloat16), shape((1, rows), jnp.int32)),
        [pltpu.VMEM((owners * block, LANES), jnp.float32)],
        [WHOLE, WHOLE, WHOLE, WHOLE],
        (WHOLE, WHOLE),
        4 * rows * owners * block * width,
        "pack",
        mib,
    )(coarse, fine, home, embeddings)
    got = lax.all_to_all(packed.reshape(peers, block, LANES), ("dp", "list"), 0, 0, tiled=True)
    old_part = lax.dynamic_slice_in_dim(coarse_old, mine * LANES, LANES, 1)
    done, new_part, over = call(
        partial(middle_kernel, cap, peers, lists_here, FINE // slices),
        (
            shape((peers, cap, LANES), jnp.bfloat16),
            shape((lists_here, LANES), jnp.bfloat16),
            shape((1, 1), jnp.float32),
        ),
        middle_scratch(cap, peers, lists_here),
        [WHOLE, WHOLE],
        (WHOLE, WHOLE, SCALAR),
        4 * total * (total + lists_here) * LANES,
        "middle",
        mib,
    )(got, old_part)
    others = tuple(
        lax.ppermute(new_part, "dp", [(i, i ^ k) for i in range(slices)]) for k in range(1, slices)
    )
    back = lax.all_to_all(done, ("dp", "list"), 0, 0, tiled=True)

    def finish(mine, placed, back, *parts):
        return call(
            partial(unpack_kernel, cap, owners, slices),
            (shape((rows, width), jnp.bfloat16), shape((lists_here, width), jnp.float32)),
            [],
            [SCALAR] + [WHOLE] * (2 + slices),
            (WHOLE, WHOLE),
            2 * rows * owners * cap * width,
            "unpack",
            mib,
        )(mine.reshape(1), placed, back.reshape(slices, owners * cap, LANES), *parts)

    return over, finish, (mine, placed, back, new_part) + others


def on_device(embeddings, coarse_id, fine_id, list_home, coarse_old):
    rows = embeddings.shape[0]
    args = (
        lax.axis_index("dp"),
        coarse_id.reshape(rows // LANES, LANES),
        fine_id.reshape(rows // LANES, LANES),
        list_home.reshape(-1, LANES),
        embeddings,
        coarse_old,
    )
    capacity, bound = 40, 96
    over, finish, parts = iterate(capacity, *args)

    def again(parts, args):
        _, finish_all, parts_all = iterate(bound, *args)
        return finish_all(*parts_all)

    return lax.cond(over[0, 0] > 0.0, again, lambda parts, args: finish(*parts), parts, args)


def solution(mesh):
    return jax.shard_map(
        on_device,
        mesh=mesh,
        in_specs=(
            P(("dp", "list"), None),
            P(("dp", "list")),
            P(("dp", "list")),
            P(),
            P("list", None),
        ),
        out_specs=(P(("dp", "list"), None), P("list", None)),
        check_vma=False,
    )
```

```python
from functools import partial

import jax
import jax.numpy as jnp
from jax import lax
from jax.experimental import pallas as pl
from jax.experimental.pallas import tpu as pltpu
from jax.sharding import PartitionSpec as P

FINE = 64
LANES = 128
KEY_ROWS = 8
HIGH = 4
STEP = 16
MIB = 1024 * 1024
WHOLE = pl.BlockSpec(memory_space=pltpu.VMEM)
SCALAR = pl.BlockSpec(memory_space=pltpu.SMEM)


def iota(shape, dim):
    return lax.broadcasted_iota(jnp.int32, shape, dim)


def ones_where(mask):
    return jnp.where(mask, 1.0, 0.0).astype(jnp.bfloat16)


def product(a, b, dims=((1,), (0,))):
    return lax.dot_general(a, b, (dims, ((), ())), preferred_element_type=jnp.float32)


def one_row(ref):
    return jnp.concatenate([ref[q : q + 1, :] for q in range(ref.shape[0])], axis=1)


def pack_kernel(cap, owners, slices, lists_here, coarse_ref, fine_ref, home_ref, rows_ref, out_ref, placed_ref, keys_ref):
    rows = rows_ref.shape[0]
    block = cap + KEY_ROWS
    peers = owners * slices
    coarse, fine = one_row(coarse_ref), one_row(fine_ref)
    table_rows = home_ref.shape[0]
    home = home_ref[...]
    column = ones_where(iota((LANES, rows), 0) == (coarse & (LANES - 1)))
    high = product((home >> 7).astype(jnp.float32).astype(jnp.bfloat16), column)
    low = product((home & 127).astype(jnp.float32).astype(jnp.bfloat16), column)
    in_row = iota((table_rows, rows), 0) == (coarse >> 7)
    position = jnp.sum(jnp.where(in_row, high * 128.0 + low, 0.0), axis=0, keepdims=True).astype(jnp.int32)
    owner = position // lists_here
    slot = position - owner * lists_here
    key = slot * FINE + fine
    target = ones_where(iota((peers, rows), 0) == owner * slices + fine // (FINE // slices))
    before = product(target, ones_where(iota((rows, rows), 0) < iota((rows, rows), 1)))
    counts = product(target, jnp.ones((rows, LANES), jnp.bfloat16))
    line, other = iota((peers, peers), 0), iota((peers, peers), 1)
    lower = ones_where((other < line) & (other // slices == line // slices))
    base = product(lower, counts.astype(jnp.bfloat16))
    base = jnp.concatenate([base] * (rows // LANES), axis=1)
    picked = jnp.where(target.astype(jnp.float32) > 0.0, before + base, 0.0)
    rank = jnp.sum(picked, axis=0, keepdims=True).astype(jnp.int32)
    fits = rank < cap
    over = jnp.max(jnp.where(fits, 0.0, 1.0))
    placed_ref[...] = jnp.where(fits, owner * cap + rank, -1)
    mine = iota((owners, rows), 0) == owner
    spread = ones_where(iota((LANES, rows), 0) == jnp.where(fits, rank, -1))
    key_high = jnp.where(mine, ((key >> 8) + 1).astype(jnp.float32), 0.0).astype(jnp.bfloat16)
    key_low = jnp.where(mine, (key & 255).astype(jnp.float32), 0.0).astype(jnp.bfloat16)
    lanes_high = product(key_high, spread, ((1,), (1,)))
    lanes_low = product(key_low, spread, ((1,), (1,)))
    line = iota((KEY_ROWS, LANES), 0)
    keys_ref[...] = jnp.zeros_like(keys_ref)
    for o in range(owners):
        tile = jnp.where(line == 0, lanes_high[o : o + 1, :], jnp.where(line == 1, lanes_low[o : o + 1, :], 0.0))
        keys_ref[o * block + cap : (o + 1) * block, :] = jnp.where(line == 2, over, tile)
    where_to = jnp.where(fits, owner * block + rank, -1)
    place = ones_where(iota((owners * block, rows), 0) == where_to)
    for pair in range(slices // 2):
        both = product(place, rows_ref[:, pair * 2 * LANES : (pair + 1) * 2 * LANES])
        for half in range(2):
            piece = both[:, half * LANES : (half + 1) * LANES] + keys_ref[...]
            out_ref[2 * pair + half, :, :] = piece.astype(jnp.bfloat16)


def middle_kernel(
    cap,
    sources,
    lists_here,
    fine_here,
    got_ref,
    old_ref,
    out_ref,
    new_ref,
    over_ref,
    aug_ref,
    key_ref,
    span_ref,
    near_ref,
    split_ref,
    total_ref,
    done_ref,
    tile_ref,
    copy_sem,
):
    for s in range(0, sources, 16):
        tile_ref[s * KEY_ROWS : (s + 16) * KEY_ROWS, :] = (
            got_ref[s : s + 16, cap : cap + KEY_ROWS, :].astype(jnp.float32).reshape(16 * KEY_ROWS, LANES)
        )
    high = tile_ref[pl.ds(0, sources, stride=KEY_ROWS), :]
    low = tile_ref[pl.ds(1, sources, stride=KEY_ROWS), :]
    over_ref[0, 0] = jnp.max(tile_ref[pl.ds(2, sources, stride=KEY_ROWS), :])
    raw = jnp.where(high > 0.0, (high - 1.0) * 256.0 + low, -1.0)
    key_ref[...] = raw.T.astype(jnp.int32)

    keys = raw.astype(jnp.int32)
    group = (keys & (FINE - 1)) // fine_here
    least = jnp.min(jnp.where(keys >= 0, group, FINE), axis=0, keepdims=True)
    most = jnp.max(jnp.where(keys >= 0, group, -1), axis=0, keepdims=True)
    blocks = span_ref.shape[0]
    lane = iota((blocks, LANES), 1)
    inside = lane // HIGH == iota((blocks, LANES), 0)
    first = jnp.min(jnp.where(inside, least, FINE), axis=1, keepdims=True)
    last = jnp.max(jnp.where(inside, most, -1), axis=1, keepdims=True)
    meet = (most >= first) & (least <= last)
    start = jnp.min(jnp.where(meet, lane, LANES), axis=1, keepdims=True)
    stop = jnp.max(jnp.where(meet, lane + 1, 0), axis=1, keepdims=True)
    span_ref[...] = jnp.where(lane == 0, start, stop)
    copy = pltpu.make_async_copy(span_ref, near_ref, copy_sem)
    copy.start()

    part = 16
    for s in range(0, sources, part):
        wide = got_ref[s : s + part, 0:cap, :].astype(jnp.float32)
        aug_ref[:, s : s + part, 0:LANES] = jnp.transpose(wide, (1, 0, 2)).astype(jnp.bfloat16)
    aug_ref[:, :, LANES : 2 * LANES] = jnp.ones((cap, sources, LANES), jnp.bfloat16)
    lists = iota((lists_here, LANES), 0)

    def list_sum(base):
        parts = [ones_where(lists == (key_ref[base + q : base + q + 1, :] >> 6)) for q in range(8)]
        return product(jnp.concatenate(parts, axis=1), aug_ref[base : base + 8].reshape(8 * sources, 2 * LANES))

    sums = sum(list_sum(t) for t in range(0, cap, 8))
    new = (old_ref[...].astype(jnp.float32) + sums[:, 0:LANES]) / (1.0 + sums[:, LANES : 2 * LANES])
    rounded = new.astype(jnp.bfloat16)
    new_ref[...] = rounded
    split_ref[:, 0:LANES] = rounded
    split_ref[:, LANES : 2 * LANES] = (new - rounded.astype(jnp.float32)).astype(jnp.bfloat16)
    copy.wait()

    step = STEP if cap > STEP else cap
    block = HIGH * sources

    def rows_of(b, carry):
        first, stop = near_ref[b, 0], near_ref[b, 1]
        start = pl.multiple_of(b * block, block)

        @pl.when(first >= stop)
        def _():
            done_ref[pl.ds(start, block), :] = jnp.zeros((block, LANES), jnp.float32)

        @pl.when(first < stop)
        def _():
            own = key_ref[pl.ds(b * HIGH, HIGH), :]
            square = jnp.concatenate([own, jnp.full((LANES - HIGH, LANES), -2, jnp.int32)], axis=0)
            turned = square.astype(jnp.float32).T.astype(jnp.int32)
            left = jnp.concatenate(
                [jnp.broadcast_to(turned[:, q : q + 1], (LANES, LANES)) for q in range(HIGH)], axis=0
            )
            narrow = left.astype(jnp.int16).reshape(block // 16, 16, LANES)

            def part_sum(t):
                wanted = first + t * step
                base = jnp.minimum(wanted, cap - step)
                parts = []
                for q in range(step):
                    row = jnp.where(base + q >= wanted, key_ref[pl.ds(base + q, 1), :], -3)
                    row = jnp.broadcast_to(row, (16, LANES)).astype(jnp.int16).reshape(1, 16, LANES)
                    same = jnp.where(narrow == row, jnp.bfloat16(1), jnp.bfloat16(0))
                    parts.append(same.reshape(block, LANES))
                right = aug_ref[pl.ds(base, step)].reshape(step * sources, 2 * LANES)
                return product(jnp.concatenate(parts, axis=1), right)

            slots = left >> 6
            parts = [ones_where(slots == iota((block, LANES), 1) + q * LANES) for q in range(lists_here // LANES)]
            centre = product(jnp.concatenate(parts, axis=1), split_ref[...])
            centre = centre[:, 0:LANES] + centre[:, LANES : 2 * LANES]
            total = part_sum(0)
            total_ref[:, 0:LANES] = total[:, 0:LANES] + centre
            total_ref[:, LANES : 2 * LANES] = total[:, LANES : 2 * LANES] + 1.0

            def more(t, inner):
                total_ref[...] += part_sum(t)
                return inner

            lax.fori_loop(1, (stop - first + step - 1) // step, more, 0)
            own_rows = aug_ref[pl.ds(b * HIGH, HIGH), :, 0:LANES].astype(jnp.float32).reshape(block, LANES)
            mean = total_ref[:, 0:LANES] / total_ref[:, LANES : 2 * LANES]
            done_ref[pl.ds(start, block), :] = own_rows - mean

        return carry

    lax.fori_loop(0, cap // HIGH, rows_of, 0)
    for s in range(0, sources, part):
        piece = jnp.concatenate(
            [done_ref[k * sources + s : k * sources + s + part, :].reshape(1, part, LANES) for k in range(cap)], axis=0
        )
        out_ref[s : s + part] = jnp.transpose(piece, (1, 0, 2)).astype(jnp.bfloat16)


def take_kernel(cap, owners, placed_ref, take_ref):
    rows = take_ref.shape[0]
    placed = placed_ref[...].astype(jnp.float32)
    lines = [placed[:, q * LANES : (q + 1) * LANES] for q in range(rows // LANES)]
    column = jnp.concatenate([jnp.broadcast_to(line, (LANES, LANES)).T for line in lines], axis=0).astype(jnp.int32)
    for r in range(owners * cap // LANES):
        take_ref[:, r * LANES : (r + 1) * LANES] = ones_where(column == iota((rows, LANES), 1) + r * LANES)


def unpack_kernel(cap, owners, slices, mine_ref, take_ref, back_ref, *refs):
    part_refs, (out_ref, new_ref) = refs[:-2], refs[-2:]
    take = take_ref[...]
    for d in range(0, slices, 2):
        both = jnp.concatenate([back_ref[d], back_ref[d + 1]], axis=1)
        out_ref[:, d * LANES : (d + 2) * LANES] = product(take, both).astype(jnp.bfloat16)
    for k, part_ref in enumerate(part_refs):
        at = pl.multiple_of((mine_ref[0] ^ k) * LANES, LANES)
        new_ref[:, pl.ds(at, LANES)] = part_ref[...].astype(jnp.float32)


def call(kernel, outs, scratch, in_specs, out_specs, flops, name, mib):
    return pl.pallas_call(
        kernel,
        out_shape=outs,
        in_specs=in_specs,
        out_specs=out_specs,
        scratch_shapes=scratch,
        compiler_params=pltpu.CompilerParams(vmem_limit_bytes=mib * MIB),
        cost_estimate=pl.CostEstimate(flops=flops, bytes_accessed=4 * MIB, transcendentals=0),
        name=name,
    )


def middle_scratch(cap, peers, lists_here):
    blocks = -(-cap // (8 * HIGH)) * 8
    return [
        pltpu.VMEM((cap, peers, 2 * LANES), jnp.bfloat16),
        pltpu.VMEM((LANES, peers), jnp.int32),
        pltpu.VMEM((blocks, LANES), jnp.int32),
        pltpu.SMEM((blocks, LANES), jnp.int32),
        pltpu.VMEM((lists_here, 2 * LANES), jnp.bfloat16),
        pltpu.VMEM((HIGH * LANES, 2 * LANES), jnp.float32),
        pltpu.VMEM((peers * cap, LANES), jnp.float32),
        pltpu.VMEM((peers * KEY_ROWS, LANES), jnp.float32),
        pltpu.SemaphoreType.DMA,
    ]


def iterate(cap, mine, coarse, fine, home, embeddings, coarse_old):
    slices, owners = lax.axis_size("dp"), lax.axis_size("list")
    peers = slices * owners
    rows, width = embeddings.shape
    lists_here = coarse_old.shape[0]
    block = cap + KEY_ROWS
    total = peers * cap
    mib = 20 if cap <= 48 else 40
    shape = jax.ShapeDtypeStruct

    packed, placed = call(
        partial(pack_kernel, cap, owners, slices, lists_here),
        (shape((slices, owners * block, LANES), jnp.bfloat16), shape((1, rows), jnp.int32)),
        [pltpu.VMEM((owners * block, LANES), jnp.float32)],
        [WHOLE, WHOLE, WHOLE, WHOLE],
        (WHOLE, WHOLE),
        4 * rows * owners * block * width,
        "pack",
        mib,
    )(coarse, fine, home, embeddings)
    got = lax.all_to_all(packed.reshape(peers, block, LANES), ("dp", "list"), 0, 0, tiled=True)
    take = call(
        partial(take_kernel, cap, owners),
        shape((rows, owners * cap), jnp.bfloat16),
        [],
        [WHOLE],
        WHOLE,
        1 << 30,
        "take",
        mib,
    )(placed)
    old_part = lax.dynamic_slice_in_dim(coarse_old, mine * LANES, LANES, 1)
    done, new_part, over = call(
        partial(middle_kernel, cap, peers, lists_here, FINE // slices),
        (
            shape((peers, cap, LANES), jnp.bfloat16),
            shape((lists_here, LANES), jnp.bfloat16),
            shape((1, 1), jnp.float32),
        ),
        middle_scratch(cap, peers, lists_here),
        [WHOLE, WHOLE],
        (WHOLE, WHOLE, SCALAR),
        4 * total * (total + lists_here) * LANES,
        "middle",
        mib,
    )(got, old_part)
    pieces = {0: new_part}
    for k in range(2, slices, 2):
        pieces[k] = lax.ppermute(new_part, "dp", [(i, i ^ k) for i in range(slices)])
    for k in range(0, slices, 2):
        pieces[k + 1] = lax.ppermute(pieces[k], "dp", [(i, i ^ 1) for i in range(slices)])
    back = lax.all_to_all(done, ("dp", "list"), 0, 0, tiled=True)

    def finish(mine, take, back, *parts):
        return call(
            partial(unpack_kernel, cap, owners, slices),
            (shape((rows, width), jnp.bfloat16), shape((lists_here, width), jnp.float32)),
            [],
            [SCALAR] + [WHOLE] * (2 + slices),
            (WHOLE, WHOLE),
            2 * rows * owners * cap * width,
            "unpack",
            mib,
        )(mine.reshape(1), take, back.reshape(slices, owners * cap, LANES), *parts)

    return over, finish, (mine, take, back) + tuple(pieces[k] for k in range(slices))


def on_device(embeddings, coarse_id, fine_id, list_home, coarse_old):
    rows = embeddings.shape[0]
    args = (
        lax.axis_index("dp"),
        coarse_id.reshape(rows // LANES, LANES),
        fine_id.reshape(rows // LANES, LANES),
        list_home.reshape(-1, LANES),
        embeddings,
        coarse_old,
    )
    capacity, bound = 40, 96
    over, finish, parts = iterate(capacity, *args)

    def again(parts, args):
        _, finish_all, parts_all = iterate(bound, *args)
        return finish_all(*parts_all)

    return lax.cond(over[0, 0] > 0.0, again, lambda parts, args: finish(*parts), parts, args)


def solution(mesh):
    return jax.shard_map(
        on_device,
        mesh=mesh,
        in_specs=(
            P(("dp", "list"), None),
            P(("dp", "list")),
            P(("dp", "list")),
            P(),
            P("list", None),
        ),
        out_specs=(P(("dp", "list"), None), P("list", None)),
        check_vma=False,
    )
```

```python
from functools import partial

import jax
import jax.numpy as jnp
from jax import lax
from jax.experimental import pallas as pl
from jax.experimental.pallas import tpu as pltpu
from jax.sharding import PartitionSpec as P

FINE = 64
LANES = 128
KEY_ROWS = 8
HIGH = 4
MIB = 1024 * 1024
WHOLE = pl.BlockSpec(memory_space=pltpu.VMEM)
SCALAR = pl.BlockSpec(memory_space=pltpu.SMEM)


def iota(shape, dim):
    return lax.broadcasted_iota(jnp.int32, shape, dim)


def ones_where(mask):
    return jnp.where(mask, 1.0, 0.0).astype(jnp.bfloat16)


def product(a, b, dims=((1,), (0,))):
    return lax.dot_general(a, b, (dims, ((), ())), preferred_element_type=jnp.float32)


def one_row(ref):
    return jnp.concatenate([ref[q : q + 1, :] for q in range(ref.shape[0])], axis=1)


def pack_kernel(cap, home_slots, owners, slices, lists_here, coarse_ref, fine_ref, home_ref, rows_ref, out_ref, placed_ref, keys_ref):
    rows = rows_ref.shape[0]
    block = cap + KEY_ROWS
    peers = owners * slices
    coarse, fine = one_row(coarse_ref), one_row(fine_ref)
    table_rows = home_ref.shape[0]
    home = home_ref[...]
    column = ones_where(iota((LANES, rows), 0) == (coarse & (LANES - 1)))
    high = product((home >> 7).astype(jnp.float32).astype(jnp.bfloat16), column)
    low = product((home & 127).astype(jnp.float32).astype(jnp.bfloat16), column)
    in_row = iota((table_rows, rows), 0) == (coarse >> 7)
    position = jnp.sum(jnp.where(in_row, high * 128.0 + low, 0.0), axis=0, keepdims=True).astype(jnp.int32)
    owner = position // lists_here
    slot = position - owner * lists_here
    key = slot * FINE + fine
    group = fine // (FINE // slices)
    target = iota((peers, rows), 0) == owner * slices + group
    mine = iota((owners, rows), 0) == owner
    earlier = ones_where(iota((rows, rows), 0) < iota((rows, rows), 1))
    within = product(ones_where(target), earlier)
    within = jnp.sum(jnp.where(target, within, 0.0), axis=0, keepdims=True).astype(jnp.int32)
    beyond = within >= home_slots
    further = product(ones_where(mine & beyond), earlier)
    further = jnp.sum(jnp.where(mine, further, 0.0), axis=0, keepdims=True).astype(jnp.int32)
    rank = jnp.where(beyond, slices * home_slots + further, group * home_slots + within)
    fits = rank < cap
    over = jnp.max(jnp.where(fits, 0.0, 1.0))
    placed_ref[...] = jnp.where(fits, owner * cap + rank, -1)
    spread = ones_where(iota((LANES, rows), 0) == jnp.where(fits, rank, -1))
    key_high = jnp.where(mine, ((key >> 8) + 1).astype(jnp.float32), 0.0).astype(jnp.bfloat16)
    key_low = jnp.where(mine, (key & 255).astype(jnp.float32), 0.0).astype(jnp.bfloat16)
    lanes_high = product(key_high, spread, ((1,), (1,)))
    lanes_low = product(key_low, spread, ((1,), (1,)))
    line = iota((KEY_ROWS, LANES), 0)
    keys_ref[...] = jnp.zeros_like(keys_ref)
    for o in range(owners):
        tile = jnp.where(line == 0, lanes_high[o : o + 1, :], jnp.where(line == 1, lanes_low[o : o + 1, :], 0.0))
        keys_ref[o * block + cap : (o + 1) * block, :] = jnp.where(line == 2, over, tile)
    where_to = jnp.where(fits, owner * block + rank, -1)
    place = ones_where(iota((owners * block, rows), 0) == where_to)
    for pair in range(slices // 2):
        both = product(place, rows_ref[:, pair * 2 * LANES : (pair + 1) * 2 * LANES])
        for half in range(2):
            piece = both[:, half * LANES : (half + 1) * LANES] + keys_ref[...]
            out_ref[2 * pair + half, :, :] = piece.astype(jnp.bfloat16)


def middle_kernel(
    cap,
    sources,
    lists_here,
    fine_here,
    got_ref,
    old_ref,
    out_ref,
    new_ref,
    over_ref,
    aug_ref,
    key_ref,
    span_ref,
    near_ref,
    split_ref,
    total_ref,
    tile_ref,
    copy_sem,
):
    for s in range(0, sources, 16):
        tile_ref[s * KEY_ROWS : (s + 16) * KEY_ROWS, :] = (
            got_ref[s : s + 16, cap : cap + KEY_ROWS, :].astype(jnp.float32).reshape(16 * KEY_ROWS, LANES)
        )
    high = tile_ref[pl.ds(0, sources, stride=KEY_ROWS), :]
    low = tile_ref[pl.ds(1, sources, stride=KEY_ROWS), :]
    over_ref[0, 0] = jnp.max(tile_ref[pl.ds(2, sources, stride=KEY_ROWS), :])
    raw = jnp.where(high > 0.0, (high - 1.0) * 256.0 + low, -1.0)
    key_ref[...] = raw.T.astype(jnp.int32)

    keys = raw.astype(jnp.int32)
    group = jnp.where(keys >= 0, (keys & (FINE - 1)) // fine_here, -1)
    present = jnp.concatenate(
        [jnp.max(jnp.where(group == g, 1.0, 0.0), axis=0, keepdims=True) for g in range(FINE // fine_here)], axis=0
    )
    chunk_of = ones_where(iota((LANES, LANES), 0) // HIGH == iota((LANES, LANES), 1))
    held = ones_where(product(present.astype(jnp.bfloat16), chunk_of) > 0.0)
    meet = product(held, held, ((0,), (0,)))
    away = iota((LANES, LANES), 0) != iota((LANES, LANES), 1)
    span_ref[...] = jnp.where((meet > 0.0) & away, 1, 0)[0 : span_ref.shape[0], :]
    number = jnp.sum(jnp.where((meet > 0.0) & away, 1, 0), axis=1, keepdims=True)[0 : span_ref.shape[0], :]
    span_ref[...] = jnp.where(iota(span_ref.shape, 1) == LANES - 1, number, span_ref[...])
    copy = pltpu.make_async_copy(span_ref, near_ref, copy_sem)
    copy.start()

    part = 16
    for s in range(0, sources, part):
        wide = got_ref[s : s + part, 0:cap, :].astype(jnp.float32)
        aug_ref[:, s : s + part, 0:LANES] = jnp.transpose(wide, (1, 0, 2)).astype(jnp.bfloat16)
    aug_ref[:, :, LANES : 2 * LANES] = jnp.ones((cap, sources, LANES), jnp.bfloat16)
    lists = iota((lists_here, LANES), 0)

    def list_sum(base):
        parts = [ones_where(lists == (key_ref[base + q : base + q + 1, :] >> 6)) for q in range(8)]
        return product(jnp.concatenate(parts, axis=1), aug_ref[base : base + 8].reshape(8 * sources, 2 * LANES))

    sums = sum(list_sum(t) for t in range(0, cap, 8))
    new = (old_ref[...].astype(jnp.float32) + sums[:, 0:LANES]) / (1.0 + sums[:, LANES : 2 * LANES])
    rounded = new.astype(jnp.bfloat16)
    new_ref[...] = rounded
    split_ref[:, 0:LANES] = rounded
    split_ref[:, LANES : 2 * LANES] = (new - rounded.astype(jnp.float32)).astype(jnp.bfloat16)
    copy.wait()

    block = HIGH * sources
    chunks = cap // HIGH

    def columns_of(b):
        own = key_ref[pl.ds(b * HIGH, HIGH), :]
        square = jnp.concatenate([own, jnp.full((LANES - HIGH, LANES), -2, jnp.int32)], axis=0)
        turned = square.astype(jnp.float32).T.astype(jnp.int32)
        return jnp.concatenate([jnp.broadcast_to(turned[:, q : q + 1], (LANES, LANES)) for q in range(HIGH)], axis=0)

    def equal_sum(left, c):
        narrow = left.astype(jnp.int16).reshape(block // 16, 16, LANES)
        parts = []
        for q in range(HIGH):
            row = jnp.broadcast_to(key_ref[pl.ds(c * HIGH + q, 1), :], (16, LANES)).astype(jnp.int16).reshape(1, 16, LANES)
            parts.append(jnp.where(narrow == row, jnp.bfloat16(1), jnp.bfloat16(0)).reshape(block, LANES))
        right = aug_ref[pl.ds(c * HIGH, HIGH)].reshape(block, 2 * LANES)
        return product(jnp.concatenate(parts, axis=1), right)

    def at_block(b):
        return pl.ds(pl.multiple_of(b * block, block), block)

    def diagonal(b):
        left = columns_of(b)
        slots = left >> 6
        parts = [ones_where(slots == iota((block, LANES), 1) + q * LANES) for q in range(lists_here // LANES)]
        centre = product(jnp.concatenate(parts, axis=1), split_ref[...])
        own = equal_sum(left, b)
        total_ref[at_block(b), 0:LANES] = own[:, 0:LANES] + centre[:, 0:LANES] + centre[:, LANES : 2 * LANES]
        total_ref[at_block(b), LANES : 2 * LANES] = own[:, LANES : 2 * LANES] + 1.0

    def both(pair, carry):
        diagonal(2 * pair)
        diagonal(2 * pair + 1)
        return carry

    lax.fori_loop(0, chunks // 2, both, 0)

    def others_of(b, carry):
        @pl.when(near_ref[b, LANES - 1] > 0)
        def _():
            def one(c, inner):
                @pl.when(near_ref[b, c] > 0)
                def _():
                    total_ref[at_block(b), :] += equal_sum(columns_of(b), c)

                return inner

            lax.fori_loop(0, chunks, one, 0)

        return carry

    lax.fori_loop(0, chunks, others_of, 0)
    for s in range(0, sources, part):
        pieces = []
        for k in range(cap):
            at = slice(k * sources + s, k * sources + s + part)
            mean = total_ref[at, 0:LANES] / total_ref[at, LANES : 2 * LANES]
            own = aug_ref[k, s : s + part, 0:LANES].astype(jnp.float32)
            pieces.append((own - mean).reshape(1, part, LANES))
        out_ref[s : s + part] = jnp.transpose(jnp.concatenate(pieces, axis=0), (1, 0, 2)).astype(jnp.bfloat16)


def take_kernel(cap, owners, placed_ref, take_ref):
    rows = take_ref.shape[0]
    placed = placed_ref[...].astype(jnp.float32)
    lines = [placed[:, q * LANES : (q + 1) * LANES] for q in range(rows // LANES)]
    column = jnp.concatenate([jnp.broadcast_to(line, (LANES, LANES)).T for line in lines], axis=0).astype(jnp.int32)
    for r in range(owners * cap // LANES):
        take_ref[:, r * LANES : (r + 1) * LANES] = ones_where(column == iota((rows, LANES), 1) + r * LANES)


def unpack_kernel(cap, owners, slices, mine_ref, take_ref, back_ref, *refs):
    part_refs, (out_ref, new_ref) = refs[:-2], refs[-2:]
    take = take_ref[...]
    for d in range(0, slices, 2):
        both = jnp.concatenate([back_ref[d], back_ref[d + 1]], axis=1)
        out_ref[:, d * LANES : (d + 2) * LANES] = product(take, both).astype(jnp.bfloat16)
    for k, part_ref in enumerate(part_refs):
        at = pl.multiple_of((mine_ref[0] ^ k) * LANES, LANES)
        new_ref[:, pl.ds(at, LANES)] = part_ref[...].astype(jnp.float32)


def call(kernel, outs, scratch, in_specs, out_specs, flops, name, mib):
    return pl.pallas_call(
        kernel,
        out_shape=outs,
        in_specs=in_specs,
        out_specs=out_specs,
        scratch_shapes=scratch,
        compiler_params=pltpu.CompilerParams(vmem_limit_bytes=mib * MIB),
        cost_estimate=pl.CostEstimate(flops=flops, bytes_accessed=4 * MIB, transcendentals=0),
        name=name,
    )


def middle_scratch(cap, peers, lists_here):
    blocks = -(-cap // (8 * HIGH)) * 8
    return [
        pltpu.VMEM((cap, peers, 2 * LANES), jnp.bfloat16),
        pltpu.VMEM((LANES, peers), jnp.int32),
        pltpu.VMEM((blocks, LANES), jnp.int32),
        pltpu.SMEM((blocks, LANES), jnp.int32),
        pltpu.VMEM((lists_here, 2 * LANES), jnp.bfloat16),
        pltpu.VMEM((peers * cap, 2 * LANES), jnp.float32),
        pltpu.VMEM((peers * KEY_ROWS, LANES), jnp.float32),
        pltpu.SemaphoreType.DMA,
    ]


def iterate(cap, home_slots, mine, coarse, fine, home, embeddings, coarse_old):
    slices, owners = lax.axis_size("dp"), lax.axis_size("list")
    peers = slices * owners
    rows, width = embeddings.shape
    lists_here = coarse_old.shape[0]
    block = cap + KEY_ROWS
    total = peers * cap
    mib = 24 if cap <= 48 else 48
    shape = jax.ShapeDtypeStruct

    packed, placed = call(
        partial(pack_kernel, cap, home_slots, owners, slices, lists_here),
        (shape((slices, owners * block, LANES), jnp.bfloat16), shape((1, rows), jnp.int32)),
        [pltpu.VMEM((owners * block, LANES), jnp.float32)],
        [WHOLE, WHOLE, WHOLE, WHOLE],
        (WHOLE, WHOLE),
        4 * rows * owners * block * width,
        "pack",
        mib,
    )(coarse, fine, home, embeddings)
    got = lax.all_to_all(packed.reshape(peers, block, LANES), ("dp", "list"), 0, 0, tiled=True)
    take = call(
        partial(take_kernel, cap, owners),
        shape((rows, owners * cap), jnp.bfloat16),
        [],
        [WHOLE],
        WHOLE,
        1 << 30,
        "take",
        mib,
    )(placed)
    old_part = lax.dynamic_slice_in_dim(coarse_old, mine * LANES, LANES, 1)
    done, new_part, over = call(
        partial(middle_kernel, cap, peers, lists_here, FINE // slices),
        (
            shape((peers, cap, LANES), jnp.bfloat16),
            shape((lists_here, LANES), jnp.bfloat16),
            shape((1, 1), jnp.float32),
        ),
        middle_scratch(cap, peers, lists_here),
        [WHOLE, WHOLE],
        (WHOLE, WHOLE, SCALAR),
        4 * total * (total + lists_here) * LANES,
        "middle",
        mib,
    )(got, old_part)
    pieces = {0: new_part}
    for k in range(2, slices, 2):
        pieces[k] = lax.ppermute(new_part, "dp", [(i, i ^ k) for i in range(slices)])
    for k in range(0, slices, 2):
        pieces[k + 1] = lax.ppermute(pieces[k], "dp", [(i, i ^ 1) for i in range(slices)])
    back = lax.all_to_all(done, ("dp", "list"), 0, 0, tiled=True)

    def finish(mine, take, back, *parts):
        return call(
            partial(unpack_kernel, cap, owners, slices),
            (shape((rows, width), jnp.bfloat16), shape((lists_here, width), jnp.float32)),
            [],
            [SCALAR] + [WHOLE] * (2 + slices),
            (WHOLE, WHOLE),
            2 * rows * owners * cap * width,
            "unpack",
            mib,
        )(mine.reshape(1), take, back.reshape(slices, owners * cap, LANES), *parts)

    return over, finish, (mine, take, back) + tuple(pieces[k] for k in range(slices))


def on_device(embeddings, coarse_id, fine_id, list_home, coarse_old):
    rows = embeddings.shape[0]
    args = (
        lax.axis_index("dp"),
        coarse_id.reshape(rows // LANES, LANES),
        fine_id.reshape(rows // LANES, LANES),
        list_home.reshape(-1, LANES),
        embeddings,
        coarse_old,
    )
    over, finish, parts = iterate(40, 4, *args)

    def again(parts, args):
        _, finish_all, parts_all = iterate(96, 12, *args)
        return finish_all(*parts_all)

    return lax.cond(over[0, 0] > 0.0, again, lambda parts, args: finish(*parts), parts, args)


def solution(mesh):
    return jax.shard_map(
        on_device,
        mesh=mesh,
        in_specs=(
            P(("dp", "list"), None),
            P(("dp", "list")),
            P(("dp", "list")),
            P(),
            P("list", None),
        ),
        out_specs=(P(("dp", "list"), None), P("list", None)),
        check_vma=False,
    )
```

```python
from functools import partial

import jax
import jax.numpy as jnp
from jax import lax
from jax.experimental import pallas as pl
from jax.experimental.pallas import tpu as pltpu
from jax.sharding import PartitionSpec as P

FINE = 64
LANES = 128
KEY_ROWS = 8
HIGH = 4
MIB = 1024 * 1024
WHOLE = pl.BlockSpec(memory_space=pltpu.VMEM)
SCALAR = pl.BlockSpec(memory_space=pltpu.SMEM)
OUTSIDE = pl.BlockSpec(memory_space=pltpu.HBM)


def iota(shape, dim):
    return lax.broadcasted_iota(jnp.int32, shape, dim)


def ones_where(mask):
    return jnp.where(mask, 1.0, 0.0).astype(jnp.bfloat16)


def product(a, b, dims=((1,), (0,))):
    return lax.dot_general(a, b, (dims, ((), ())), preferred_element_type=jnp.float32)


def one_row(ref):
    return jnp.concatenate([ref[q : q + 1, :] for q in range(ref.shape[0])], axis=1)


def pack_kernel(cap, home_slots, owners, slices, lists_here, coarse_ref, fine_ref, home_ref, far_ref, out_ref, placed_ref, keys_ref, rows_ref, sent_ref, sems):
    rows = rows_ref.shape[0]
    fetch = pltpu.make_async_copy(far_ref, rows_ref, sems.at[slices // 2])
    fetch.start()
    block = cap + KEY_ROWS
    peers = owners * slices
    coarse, fine = one_row(coarse_ref), one_row(fine_ref)
    table_rows = home_ref.shape[0]
    home = home_ref[...]
    column = ones_where(iota((LANES, rows), 0) == (coarse & (LANES - 1)))
    high = product((home >> 7).astype(jnp.float32).astype(jnp.bfloat16), column)
    low = product((home & 127).astype(jnp.float32).astype(jnp.bfloat16), column)
    in_row = iota((table_rows, rows), 0) == (coarse >> 7)
    position = jnp.sum(jnp.where(in_row, high * 128.0 + low, 0.0), axis=0, keepdims=True).astype(jnp.int32)
    owner = position // lists_here
    slot = position - owner * lists_here
    key = slot * FINE + fine
    group = fine // (FINE // slices)
    target = iota((peers, rows), 0) == owner * slices + group
    mine = iota((owners, rows), 0) == owner
    earlier = ones_where(iota((rows, rows), 0) < iota((rows, rows), 1))
    within = product(ones_where(target), earlier)
    within = jnp.sum(jnp.where(target, within, 0.0), axis=0, keepdims=True).astype(jnp.int32)
    beyond = within >= home_slots
    further = product(ones_where(mine & beyond), earlier)
    further = jnp.sum(jnp.where(mine, further, 0.0), axis=0, keepdims=True).astype(jnp.int32)
    rank = jnp.where(beyond, slices * home_slots + further, group * home_slots + within)
    fits = rank < cap
    over = jnp.max(jnp.where(fits, 0.0, 1.0))
    placed_ref[...] = jnp.where(fits, owner * cap + rank, -1)
    spread = ones_where(iota((LANES, rows), 0) == jnp.where(fits, rank, -1))
    key_high = jnp.where(mine, ((key >> 8) + 1).astype(jnp.float32), 0.0).astype(jnp.bfloat16)
    key_low = jnp.where(mine, (key & 255).astype(jnp.float32), 0.0).astype(jnp.bfloat16)
    lanes_high = product(key_high, spread, ((1,), (1,)))
    lanes_low = product(key_low, spread, ((1,), (1,)))
    line = iota((KEY_ROWS, LANES), 0)
    keys_ref[...] = jnp.zeros_like(keys_ref)
    for o in range(owners):
        tile = jnp.where(line == 0, lanes_high[o : o + 1, :], jnp.where(line == 1, lanes_low[o : o + 1, :], 0.0))
        keys_ref[o * block + cap : (o + 1) * block, :] = jnp.where(line == 2, over, tile)
    where_to = jnp.where(fits, owner * block + rank, -1)
    place = ones_where(iota((owners * block, rows), 0) == where_to)
    fetch.wait()
    copies = []
    for pair in range(slices // 2):
        both = product(place, rows_ref[:, pair * 2 * LANES : (pair + 1) * 2 * LANES])
        for half in range(2):
            piece = both[:, half * LANES : (half + 1) * LANES] + keys_ref[...]
            sent_ref[2 * pair + half, :, :] = piece.astype(jnp.bfloat16)
        at = pl.ds(2 * pair, 2)
        copies.append(pltpu.make_async_copy(sent_ref.at[at], out_ref.at[at], sems.at[pair]))
        copies[-1].start()
    for copy in copies:
        copy.wait()


def middle_kernel(
    cap,
    sources,
    lists_here,
    fine_here,
    got_ref,
    old_ref,
    out_ref,
    new_ref,
    over_ref,
    aug_ref,
    key_ref,
    span_ref,
    near_ref,
    split_ref,
    total_ref,
    tile_ref,
    sent_ref,
    copy_sem,
    sems,
):
    for s in range(0, sources, 16):
        tile_ref[s * KEY_ROWS : (s + 16) * KEY_ROWS, :] = (
            got_ref[s : s + 16, cap : cap + KEY_ROWS, :].astype(jnp.float32).reshape(16 * KEY_ROWS, LANES)
        )
    high = tile_ref[pl.ds(0, sources, stride=KEY_ROWS), :]
    low = tile_ref[pl.ds(1, sources, stride=KEY_ROWS), :]
    over_ref[0, 0] = jnp.max(tile_ref[pl.ds(2, sources, stride=KEY_ROWS), :])
    raw = jnp.where(high > 0.0, (high - 1.0) * 256.0 + low, -1.0)
    key_ref[...] = raw.T.astype(jnp.int32)

    keys = raw.astype(jnp.int32)
    group = jnp.where(keys >= 0, (keys & (FINE - 1)) // fine_here, -1)
    present = jnp.concatenate(
        [jnp.max(jnp.where(group == g, 1.0, 0.0), axis=0, keepdims=True) for g in range(FINE // fine_here)], axis=0
    )
    chunk_of = ones_where(iota((LANES, LANES), 0) // HIGH == iota((LANES, LANES), 1))
    held = ones_where(product(present.astype(jnp.bfloat16), chunk_of) > 0.0)
    meet = product(held, held, ((0,), (0,)))
    away = iota((LANES, LANES), 0) != iota((LANES, LANES), 1)
    span_ref[...] = jnp.where((meet > 0.0) & away, 1, 0)[0 : span_ref.shape[0], :]
    number = jnp.sum(jnp.where((meet > 0.0) & away, 1, 0), axis=1, keepdims=True)[0 : span_ref.shape[0], :]
    span_ref[...] = jnp.where(iota(span_ref.shape, 1) == LANES - 1, number, span_ref[...])
    copy = pltpu.make_async_copy(span_ref, near_ref, copy_sem)
    copy.start()

    part = 16
    for s in range(0, sources, part):
        wide = got_ref[s : s + part, 0:cap, :].astype(jnp.float32)
        aug_ref[:, s : s + part, 0:LANES] = jnp.transpose(wide, (1, 0, 2)).astype(jnp.bfloat16)
    aug_ref[:, :, LANES : 2 * LANES] = jnp.ones((cap, sources, LANES), jnp.bfloat16)
    lists = iota((lists_here, LANES), 0)

    def list_sum(base):
        parts = [ones_where(lists == (key_ref[base + q : base + q + 1, :] >> 6)) for q in range(8)]
        return product(jnp.concatenate(parts, axis=1), aug_ref[base : base + 8].reshape(8 * sources, 2 * LANES))

    sums = sum(list_sum(t) for t in range(0, cap, 8))
    new = (old_ref[...].astype(jnp.float32) + sums[:, 0:LANES]) / (1.0 + sums[:, LANES : 2 * LANES])
    rounded = new.astype(jnp.bfloat16)
    new_ref[...] = rounded
    split_ref[:, 0:LANES] = rounded
    split_ref[:, LANES : 2 * LANES] = (new - rounded.astype(jnp.float32)).astype(jnp.bfloat16)
    copy.wait()

    block = HIGH * sources
    chunks = cap // HIGH

    def columns_of(b):
        own = key_ref[pl.ds(b * HIGH, HIGH), :]
        square = jnp.concatenate([own, jnp.full((LANES - HIGH, LANES), -2, jnp.int32)], axis=0)
        turned = square.astype(jnp.float32).T.astype(jnp.int32)
        return jnp.concatenate([jnp.broadcast_to(turned[:, q : q + 1], (LANES, LANES)) for q in range(HIGH)], axis=0)

    def equal_sum(left, c):
        narrow = left.astype(jnp.int16).reshape(block // 16, 16, LANES)
        parts = []
        for q in range(HIGH):
            row = jnp.broadcast_to(key_ref[pl.ds(c * HIGH + q, 1), :], (16, LANES)).astype(jnp.int16).reshape(1, 16, LANES)
            parts.append(jnp.where(narrow == row, jnp.bfloat16(1), jnp.bfloat16(0)).reshape(block, LANES))
        right = aug_ref[pl.ds(c * HIGH, HIGH)].reshape(block, 2 * LANES)
        return product(jnp.concatenate(parts, axis=1), right)

    def at_block(b):
        return pl.ds(pl.multiple_of(b * block, block), block)

    def diagonal(b):
        left = columns_of(b)
        slots = left >> 6
        parts = [ones_where(slots == iota((block, LANES), 1) + q * LANES) for q in range(lists_here // LANES)]
        centre = product(jnp.concatenate(parts, axis=1), split_ref[...])
        own = equal_sum(left, b)
        total_ref[at_block(b), 0:LANES] = own[:, 0:LANES] + centre[:, 0:LANES] + centre[:, LANES : 2 * LANES]
        total_ref[at_block(b), LANES : 2 * LANES] = own[:, LANES : 2 * LANES] + 1.0

    def both(pair, carry):
        diagonal(2 * pair)
        diagonal(2 * pair + 1)
        return carry

    lax.fori_loop(0, chunks // 2, both, 0)

    def others_of(b, carry):
        @pl.when(near_ref[b, LANES - 1] > 0)
        def _():
            def one(c, inner):
                @pl.when(near_ref[b, c] > 0)
                def _():
                    total_ref[at_block(b), :] += equal_sum(columns_of(b), c)

                return inner

            lax.fori_loop(0, chunks, one, 0)

        return carry

    lax.fori_loop(0, chunks, others_of, 0)
    copies = []
    for s in range(0, sources, part):
        pieces = []
        for k in range(cap):
            at = slice(k * sources + s, k * sources + s + part)
            mean = total_ref[at, 0:LANES] / total_ref[at, LANES : 2 * LANES]
            own = aug_ref[k, s : s + part, 0:LANES].astype(jnp.float32)
            pieces.append((own - mean).reshape(1, part, LANES))
        sent_ref[s : s + part] = jnp.transpose(jnp.concatenate(pieces, axis=0), (1, 0, 2)).astype(jnp.bfloat16)
        at = pl.ds(s, part)
        copies.append(pltpu.make_async_copy(sent_ref.at[at], out_ref.at[at], sems.at[s // part]))
        copies[-1].start()
    for copy in copies:
        copy.wait()


def take_kernel(cap, owners, placed_ref, take_ref):
    rows = take_ref.shape[0]
    placed = placed_ref[...].astype(jnp.float32)
    lines = [placed[:, q * LANES : (q + 1) * LANES] for q in range(rows // LANES)]
    column = jnp.concatenate([jnp.broadcast_to(line, (LANES, LANES)).T for line in lines], axis=0).astype(jnp.int32)
    for r in range(owners * cap // LANES):
        take_ref[:, r * LANES : (r + 1) * LANES] = ones_where(column == iota((rows, LANES), 1) + r * LANES)


def unpack_kernel(cap, owners, slices, mine_ref, take_ref, back_ref, *refs):
    part_refs, (out_ref, new_ref, wide_ref, sent_ref, sems) = refs[:-5], refs[-5:]
    copies = []
    for k, part_ref in enumerate(part_refs):
        wide_ref[k] = part_ref[...].astype(jnp.float32)
        at = pl.multiple_of((mine_ref[0] ^ k) * LANES, LANES)
        copies.append(pltpu.make_async_copy(wide_ref.at[k], new_ref.at[:, pl.ds(at, LANES)], sems.at[k]))
        copies[-1].start()
    take = take_ref[...]
    for d in range(0, slices, 2):
        both = jnp.concatenate([back_ref[d], back_ref[d + 1]], axis=1)
        at = pl.ds(d * LANES, 2 * LANES)
        sent_ref[:, at] = product(take, both).astype(jnp.bfloat16)
        copies.append(pltpu.make_async_copy(sent_ref.at[:, at], out_ref.at[:, at], sems.at[slices + d // 2]))
        copies[-1].start()
    for copy in copies:
        copy.wait()


def call(kernel, outs, scratch, in_specs, out_specs, flops, name, mib):
    return pl.pallas_call(
        kernel,
        out_shape=outs,
        in_specs=in_specs,
        out_specs=out_specs,
        scratch_shapes=scratch,
        compiler_params=pltpu.CompilerParams(vmem_limit_bytes=mib * MIB),
        cost_estimate=pl.CostEstimate(flops=flops, bytes_accessed=4 * MIB, transcendentals=0),
        name=name,
    )


def middle_scratch(cap, peers, lists_here):
    blocks = -(-cap // (8 * HIGH)) * 8
    return [
        pltpu.VMEM((cap, peers, 2 * LANES), jnp.bfloat16),
        pltpu.VMEM((LANES, peers), jnp.int32),
        pltpu.VMEM((blocks, LANES), jnp.int32),
        pltpu.SMEM((blocks, LANES), jnp.int32),
        pltpu.VMEM((lists_here, 2 * LANES), jnp.bfloat16),
        pltpu.VMEM((peers * cap, 2 * LANES), jnp.float32),
        pltpu.VMEM((peers * KEY_ROWS, LANES), jnp.float32),
        pltpu.VMEM((peers, cap, LANES), jnp.bfloat16),
        pltpu.SemaphoreType.DMA,
        pltpu.SemaphoreType.DMA((peers // 16,)),
    ]


def iterate(cap, home_slots, mine, coarse, fine, home, embeddings, coarse_old):
    slices, owners = lax.axis_size("dp"), lax.axis_size("list")
    peers = slices * owners
    rows, width = embeddings.shape
    lists_here = coarse_old.shape[0]
    block = cap + KEY_ROWS
    total = peers * cap
    mib = 26 if cap <= 48 else 56
    shape = jax.ShapeDtypeStruct

    packed, placed = call(
        partial(pack_kernel, cap, home_slots, owners, slices, lists_here),
        (shape((slices, owners * block, LANES), jnp.bfloat16), shape((1, rows), jnp.int32)),
        [
            pltpu.VMEM((owners * block, LANES), jnp.float32),
            pltpu.VMEM((rows, width), jnp.bfloat16),
            pltpu.VMEM((slices, owners * block, LANES), jnp.bfloat16),
            pltpu.SemaphoreType.DMA((slices // 2 + 1,)),
        ],
        [WHOLE, WHOLE, WHOLE, OUTSIDE],
        (OUTSIDE, WHOLE),
        4 * rows * owners * block * width,
        "pack",
        mib,
    )(coarse, fine, home, embeddings)
    got = lax.all_to_all(packed.reshape(peers, block, LANES), ("dp", "list"), 0, 0, tiled=True)
    take = call(
        partial(take_kernel, cap, owners),
        shape((rows, owners * cap), jnp.bfloat16),
        [],
        [WHOLE],
        WHOLE,
        1 << 30,
        "take",
        mib,
    )(placed)
    old_part = lax.dynamic_slice_in_dim(coarse_old, mine * LANES, LANES, 1)
    done, new_part, over = call(
        partial(middle_kernel, cap, peers, lists_here, FINE // slices),
        (
            shape((peers, cap, LANES), jnp.bfloat16),
            shape((lists_here, LANES), jnp.bfloat16),
            shape((1, 1), jnp.float32),
        ),
        middle_scratch(cap, peers, lists_here),
        [WHOLE, WHOLE],
        (OUTSIDE, WHOLE, SCALAR),
        4 * total * (total + lists_here) * LANES,
        "middle",
        mib,
    )(got, old_part)
    pieces = {0: new_part}
    for k in range(2, slices, 2):
        pieces[k] = lax.ppermute(new_part, "dp", [(i, i ^ k) for i in range(slices)])
    for k in range(0, slices, 2):
        pieces[k + 1] = lax.ppermute(pieces[k], "dp", [(i, i ^ 1) for i in range(slices)])
    back = lax.all_to_all(done, ("dp", "list"), 0, 0, tiled=True)

    def finish(mine, take, back, *parts):
        return call(
            partial(unpack_kernel, cap, owners, slices),
            (shape((rows, width), jnp.bfloat16), shape((lists_here, width), jnp.float32)),
            [
                pltpu.VMEM((slices, lists_here, LANES), jnp.float32),
                pltpu.VMEM((rows, width), jnp.bfloat16),
                pltpu.SemaphoreType.DMA((slices + slices // 2,)),
            ],
            [SCALAR] + [WHOLE] * (2 + slices),
            (OUTSIDE, OUTSIDE),
            2 * rows * owners * cap * width,
            "unpack",
            mib,
        )(mine.reshape(1), take, back.reshape(slices, owners * cap, LANES), *parts)

    return over, finish, (mine, take, back) + tuple(pieces[k] for k in range(slices))


def on_device(embeddings, coarse_id, fine_id, list_home, coarse_old):
    rows = embeddings.shape[0]
    args = (
        lax.axis_index("dp"),
        coarse_id.reshape(rows // LANES, LANES),
        fine_id.reshape(rows // LANES, LANES),
        list_home.reshape(-1, LANES),
        embeddings,
        coarse_old,
    )
    over, finish, parts = iterate(40, 4, *args)

    def again(parts, args):
        _, finish_all, parts_all = iterate(96, 12, *args)
        return finish_all(*parts_all)

    return lax.cond(over[0, 0] > 0.0, again, lambda parts, args: finish(*parts), parts, args)


def solution(mesh):
    return jax.shard_map(
        on_device,
        mesh=mesh,
        in_specs=(
            P(("dp", "list"), None),
            P(("dp", "list")),
            P(("dp", "list")),
            P(),
            P("list", None),
        ),
        out_specs=(P(("dp", "list"), None), P("list", None)),
        check_vma=False,
    )
```

```python
from functools import partial

import jax
import jax.numpy as jnp
from jax import lax
from jax.experimental import pallas as pl
from jax.experimental.pallas import tpu as pltpu
from jax.sharding import PartitionSpec as P

FINE = 64
LANES = 128
KEY_ROWS = 8
HIGH = 4
MIB = 1024 * 1024
WHOLE = pl.BlockSpec(memory_space=pltpu.VMEM)
SCALAR = pl.BlockSpec(memory_space=pltpu.SMEM)
OUTSIDE = pl.BlockSpec(memory_space=pltpu.HBM)


def iota(shape, dim):
    return lax.broadcasted_iota(jnp.int32, shape, dim)


def ones_where(mask):
    return jnp.where(mask, 1.0, 0.0).astype(jnp.bfloat16)


def product(a, b, dims=((1,), (0,))):
    return lax.dot_general(a, b, (dims, ((), ())), preferred_element_type=jnp.float32)


def one_row(ref):
    return jnp.concatenate([ref[q : q + 1, :] for q in range(ref.shape[0])], axis=1)


def pack_kernel(cap, home_slots, owners, slices, lists_here, coarse_ref, fine_ref, home_ref, rows_ref, out_ref, placed_ref, keys_ref, sent_ref, sems):
    rows = rows_ref.shape[0]
    block = cap + KEY_ROWS
    peers = owners * slices
    coarse, fine = one_row(coarse_ref), one_row(fine_ref)
    table_rows = home_ref.shape[0]
    home = home_ref[...]
    column = ones_where(iota((LANES, rows), 0) == (coarse & (LANES - 1)))
    high = product((home >> 7).astype(jnp.float32).astype(jnp.bfloat16), column)
    low = product((home & 127).astype(jnp.float32).astype(jnp.bfloat16), column)
    in_row = iota((table_rows, rows), 0) == (coarse >> 7)
    position = jnp.sum(jnp.where(in_row, high * 128.0 + low, 0.0), axis=0, keepdims=True).astype(jnp.int32)
    owner = position // lists_here
    slot = position - owner * lists_here
    key = slot * FINE + fine
    group = fine // (FINE // slices)
    target = iota((peers, rows), 0) == owner * slices + group
    mine = iota((owners, rows), 0) == owner
    earlier = ones_where(iota((rows, rows), 0) < iota((rows, rows), 1))
    within = product(ones_where(target), earlier)
    within = jnp.sum(jnp.where(target, within, 0.0), axis=0, keepdims=True).astype(jnp.int32)
    beyond = within >= home_slots
    further = product(ones_where(mine & beyond), earlier)
    further = jnp.sum(jnp.where(mine, further, 0.0), axis=0, keepdims=True).astype(jnp.int32)
    rank = jnp.where(beyond, slices * home_slots + further, group * home_slots + within)
    fits = rank < cap
    over = jnp.max(jnp.where(fits, 0.0, 1.0))
    placed_ref[...] = jnp.where(fits, owner * cap + rank, -1)
    spread = ones_where(iota((LANES, rows), 0) == jnp.where(fits, rank, -1))
    key_high = jnp.where(mine, ((key >> 8) + 1).astype(jnp.float32), 0.0).astype(jnp.bfloat16)
    key_low = jnp.where(mine, (key & 255).astype(jnp.float32), 0.0).astype(jnp.bfloat16)
    lanes_high = product(key_high, spread, ((1,), (1,)))
    lanes_low = product(key_low, spread, ((1,), (1,)))
    line = iota((KEY_ROWS, LANES), 0)
    keys_ref[...] = jnp.zeros_like(keys_ref)
    for o in range(owners):
        tile = jnp.where(line == 0, lanes_high[o : o + 1, :], jnp.where(line == 1, lanes_low[o : o + 1, :], 0.0))
        keys_ref[o * block + cap : (o + 1) * block, :] = jnp.where(line == 2, over, tile)
    where_to = jnp.where(fits, owner * block + rank, -1)
    place = ones_where(iota((owners * block, rows), 0) == where_to)
    copies = []
    for pair in range(slices // 2):
        both = product(place, rows_ref[:, pair * 2 * LANES : (pair + 1) * 2 * LANES])
        for half in range(2):
            piece = both[:, half * LANES : (half + 1) * LANES] + keys_ref[...]
            sent_ref[2 * pair + half, :, :] = piece.astype(jnp.bfloat16)
        at = pl.ds(2 * pair, 2)
        copies.append(pltpu.make_async_copy(sent_ref.at[at], out_ref.at[at], sems.at[pair]))
        copies[-1].start()
    for copy in copies:
        copy.wait()


def middle_kernel(
    cap,
    sources,
    lists_here,
    fine_here,
    got_ref,
    old_ref,
    out_ref,
    new_ref,
    over_ref,
    aug_ref,
    key_ref,
    span_ref,
    near_ref,
    split_ref,
    total_ref,
    tile_ref,
    copy_sem,
):
    for s in range(0, sources, 16):
        tile_ref[s * KEY_ROWS : (s + 16) * KEY_ROWS, :] = (
            got_ref[s : s + 16, cap : cap + KEY_ROWS, :].astype(jnp.float32).reshape(16 * KEY_ROWS, LANES)
        )
    high = tile_ref[pl.ds(0, sources, stride=KEY_ROWS), :]
    low = tile_ref[pl.ds(1, sources, stride=KEY_ROWS), :]
    over_ref[0, 0] = jnp.max(tile_ref[pl.ds(2, sources, stride=KEY_ROWS), :])
    raw = jnp.where(high > 0.0, (high - 1.0) * 256.0 + low, -1.0)
    key_ref[...] = raw.T.astype(jnp.int32)

    keys = raw.astype(jnp.int32)
    group = jnp.where(keys >= 0, (keys & (FINE - 1)) // fine_here, -1)
    present = jnp.concatenate(
        [jnp.max(jnp.where(group == g, 1.0, 0.0), axis=0, keepdims=True) for g in range(FINE // fine_here)], axis=0
    )
    chunk_of = ones_where(iota((LANES, LANES), 0) // HIGH == iota((LANES, LANES), 1))
    held = ones_where(product(present.astype(jnp.bfloat16), chunk_of) > 0.0)
    meet = product(held, held, ((0,), (0,)))
    away = iota((LANES, LANES), 0) != iota((LANES, LANES), 1)
    span_ref[...] = jnp.where((meet > 0.0) & away, 1, 0)[0 : span_ref.shape[0], :]
    number = jnp.sum(jnp.where((meet > 0.0) & away, 1, 0), axis=1, keepdims=True)[0 : span_ref.shape[0], :]
    span_ref[...] = jnp.where(iota(span_ref.shape, 1) == LANES - 1, number, span_ref[...])
    copy = pltpu.make_async_copy(span_ref, near_ref, copy_sem)
    copy.start()

    part = 16
    for s in range(0, sources, part):
        wide = got_ref[s : s + part, 0:cap, :].astype(jnp.float32)
        aug_ref[:, s : s + part, 0:LANES] = jnp.transpose(wide, (1, 0, 2)).astype(jnp.bfloat16)
    aug_ref[:, :, LANES : 2 * LANES] = jnp.ones((cap, sources, LANES), jnp.bfloat16)
    lists = iota((lists_here, LANES), 0)

    def list_sum(base):
        parts = [ones_where(lists == (key_ref[base + q : base + q + 1, :] >> 6)) for q in range(8)]
        return product(jnp.concatenate(parts, axis=1), aug_ref[base : base + 8].reshape(8 * sources, 2 * LANES))

    sums = sum(list_sum(t) for t in range(0, cap, 8))
    new = (old_ref[...].astype(jnp.float32) + sums[:, 0:LANES]) / (1.0 + sums[:, LANES : 2 * LANES])
    rounded = new.astype(jnp.bfloat16)
    new_ref[...] = rounded
    split_ref[:, 0:LANES] = rounded
    split_ref[:, LANES : 2 * LANES] = (new - rounded.astype(jnp.float32)).astype(jnp.bfloat16)
    copy.wait()

    block = HIGH * sources
    chunks = cap // HIGH

    def columns_of(b):
        own = key_ref[pl.ds(b * HIGH, HIGH), :]
        square = jnp.concatenate([own, jnp.full((LANES - HIGH, LANES), -2, jnp.int32)], axis=0)
        turned = square.astype(jnp.float32).T.astype(jnp.int32)
        return jnp.concatenate([jnp.broadcast_to(turned[:, q : q + 1], (LANES, LANES)) for q in range(HIGH)], axis=0)

    def equal_sum(left, c):
        narrow = left.astype(jnp.int16).reshape(block // 16, 16, LANES)
        parts = []
        for q in range(HIGH):
            row = jnp.broadcast_to(key_ref[pl.ds(c * HIGH + q, 1), :], (16, LANES)).astype(jnp.int16).reshape(1, 16, LANES)
            parts.append(jnp.where(narrow == row, jnp.bfloat16(1), jnp.bfloat16(0)).reshape(block, LANES))
        right = aug_ref[pl.ds(c * HIGH, HIGH)].reshape(block, 2 * LANES)
        return product(jnp.concatenate(parts, axis=1), right)

    def at_block(b):
        return pl.ds(pl.multiple_of(b * block, block), block)

    def diagonal(b):
        left = columns_of(b)
        slots = left >> 6
        parts = [ones_where(slots == iota((block, LANES), 1) + q * LANES) for q in range(lists_here // LANES)]
        centre = product(jnp.concatenate(parts, axis=1), split_ref[...])
        own = equal_sum(left, b)
        total_ref[at_block(b), 0:LANES] = own[:, 0:LANES] + centre[:, 0:LANES] + centre[:, LANES : 2 * LANES]
        total_ref[at_block(b), LANES : 2 * LANES] = own[:, LANES : 2 * LANES] + 1.0

    def both(pair, carry):
        diagonal(2 * pair)
        diagonal(2 * pair + 1)
        return carry

    lax.fori_loop(0, chunks // 2, both, 0)

    def others_of(b, carry):
        @pl.when(near_ref[b, LANES - 1] > 0)
        def _():
            def one(c, inner):
                @pl.when(near_ref[b, c] > 0)
                def _():
                    total_ref[at_block(b), :] += equal_sum(columns_of(b), c)

                return inner

            lax.fori_loop(0, chunks, one, 0)

        return carry

    lax.fori_loop(0, chunks, others_of, 0)
    for s in range(0, sources, part):
        pieces = []
        for k in range(cap):
            at = slice(k * sources + s, k * sources + s + part)
            mean = total_ref[at, 0:LANES] / total_ref[at, LANES : 2 * LANES]
            own = aug_ref[k, s : s + part, 0:LANES].astype(jnp.float32)
            pieces.append((own - mean).reshape(1, part, LANES))
        out_ref[s : s + part] = jnp.transpose(jnp.concatenate(pieces, axis=0), (1, 0, 2)).astype(jnp.bfloat16)


def take_kernel(cap, owners, placed_ref, take_ref):
    rows = take_ref.shape[0]
    placed = placed_ref[...].astype(jnp.float32)
    lines = [placed[:, q * LANES : (q + 1) * LANES] for q in range(rows // LANES)]
    column = jnp.concatenate([jnp.broadcast_to(line, (LANES, LANES)).T for line in lines], axis=0).astype(jnp.int32)
    for r in range(owners * cap // LANES):
        take_ref[:, r * LANES : (r + 1) * LANES] = ones_where(column == iota((rows, LANES), 1) + r * LANES)


def unpack_kernel(cap, owners, slices, mine_ref, take_ref, back_ref, *refs):
    part_refs, (out_ref, new_ref, wide_ref, sent_ref, sems) = refs[:-5], refs[-5:]
    copies = []
    for k, part_ref in enumerate(part_refs):
        wide_ref[k] = part_ref[...].astype(jnp.float32)
        at = pl.multiple_of((mine_ref[0] ^ k) * LANES, LANES)
        copies.append(pltpu.make_async_copy(wide_ref.at[k], new_ref.at[:, pl.ds(at, LANES)], sems.at[k]))
        copies[-1].start()
    take = take_ref[...]
    for d in range(0, slices, 2):
        both = jnp.concatenate([back_ref[d], back_ref[d + 1]], axis=1)
        at = pl.ds(d * LANES, 2 * LANES)
        sent_ref[:, at] = product(take, both).astype(jnp.bfloat16)
        copies.append(pltpu.make_async_copy(sent_ref.at[:, at], out_ref.at[:, at], sems.at[slices + d // 2]))
        copies[-1].start()
    for copy in copies:
        copy.wait()


def call(kernel, outs, scratch, in_specs, out_specs, flops, name, mib):
    return pl.pallas_call(
        kernel,
        out_shape=outs,
        in_specs=in_specs,
        out_specs=out_specs,
        scratch_shapes=scratch,
        compiler_params=pltpu.CompilerParams(vmem_limit_bytes=mib * MIB),
        cost_estimate=pl.CostEstimate(flops=flops, bytes_accessed=4 * MIB, transcendentals=0),
        name=name,
    )


def middle_scratch(cap, peers, lists_here):
    blocks = -(-cap // (8 * HIGH)) * 8
    return [
        pltpu.VMEM((cap, peers, 2 * LANES), jnp.bfloat16),
        pltpu.VMEM((LANES, peers), jnp.int32),
        pltpu.VMEM((blocks, LANES), jnp.int32),
        pltpu.SMEM((blocks, LANES), jnp.int32),
        pltpu.VMEM((lists_here, 2 * LANES), jnp.bfloat16),
        pltpu.VMEM((peers * cap, 2 * LANES), jnp.float32),
        pltpu.VMEM((peers * KEY_ROWS, LANES), jnp.float32),
        pltpu.SemaphoreType.DMA,
    ]


def iterate(cap, home_slots, mine, coarse, fine, home, embeddings, coarse_old):
    slices, owners = lax.axis_size("dp"), lax.axis_size("list")
    peers = slices * owners
    rows, width = embeddings.shape
    lists_here = coarse_old.shape[0]
    block = cap + KEY_ROWS
    total = peers * cap
    mib = 26 if cap <= 48 else 56
    shape = jax.ShapeDtypeStruct

    packed, placed = call(
        partial(pack_kernel, cap, home_slots, owners, slices, lists_here),
        (shape((slices, owners * block, LANES), jnp.bfloat16), shape((1, rows), jnp.int32)),
        [
            pltpu.VMEM((owners * block, LANES), jnp.float32),
            pltpu.VMEM((slices, owners * block, LANES), jnp.bfloat16),
            pltpu.SemaphoreType.DMA((slices // 2,)),
        ],
        [WHOLE, WHOLE, WHOLE, WHOLE],
        (OUTSIDE, WHOLE),
        4 * rows * owners * block * width,
        "pack",
        mib,
    )(coarse, fine, home, embeddings)
    got = lax.all_to_all(packed.reshape(peers, block, LANES), ("dp", "list"), 0, 0, tiled=True)
    take = call(
        partial(take_kernel, cap, owners),
        shape((rows, owners * cap), jnp.bfloat16),
        [],
        [WHOLE],
        WHOLE,
        1 << 30,
        "take",
        mib,
    )(placed)
    old_part = lax.dynamic_slice_in_dim(coarse_old, mine * LANES, LANES, 1)
    done, new_part, over = call(
        partial(middle_kernel, cap, peers, lists_here, FINE // slices),
        (
            shape((peers, cap, LANES), jnp.bfloat16),
            shape((lists_here, LANES), jnp.bfloat16),
            shape((1, 1), jnp.float32),
        ),
        middle_scratch(cap, peers, lists_here),
        [WHOLE, WHOLE],
        (WHOLE, WHOLE, SCALAR),
        4 * total * (total + lists_here) * LANES,
        "middle",
        mib,
    )(got, old_part)
    pieces = {0: new_part}
    for k in range(2, slices, 2):
        pieces[k] = lax.ppermute(new_part, "dp", [(i, i ^ k) for i in range(slices)])
    for k in range(0, slices, 2):
        pieces[k + 1] = lax.ppermute(pieces[k], "dp", [(i, i ^ 1) for i in range(slices)])
    back = lax.all_to_all(done, ("dp", "list"), 0, 0, tiled=True)

    def finish(mine, take, back, *parts):
        return call(
            partial(unpack_kernel, cap, owners, slices),
            (shape((rows, width), jnp.bfloat16), shape((lists_here, width), jnp.float32)),
            [
                pltpu.VMEM((slices, lists_here, LANES), jnp.float32),
                pltpu.VMEM((rows, width), jnp.bfloat16),
                pltpu.SemaphoreType.DMA((slices + slices // 2,)),
            ],
            [SCALAR] + [WHOLE] * (2 + slices),
            (OUTSIDE, OUTSIDE),
            2 * rows * owners * cap * width,
            "unpack",
            mib,
        )(mine.reshape(1), take, back.reshape(slices, owners * cap, LANES), *parts)

    return over, finish, (mine, take, back) + tuple(pieces[k] for k in range(slices))


def on_device(embeddings, coarse_id, fine_id, list_home, coarse_old):
    rows = embeddings.shape[0]
    args = (
        lax.axis_index("dp"),
        coarse_id.reshape(rows // LANES, LANES),
        fine_id.reshape(rows // LANES, LANES),
        list_home.reshape(-1, LANES),
        embeddings,
        coarse_old,
    )
    over, finish, parts = iterate(40, 4, *args)

    def again(parts, args):
        _, finish_all, parts_all = iterate(96, 12, *args)
        return finish_all(*parts_all)

    return lax.cond(over[0, 0] > 0.0, again, lambda parts, args: finish(*parts), parts, args)


def solution(mesh):
    return jax.shard_map(
        on_device,
        mesh=mesh,
        in_specs=(
            P(("dp", "list"), None),
            P(("dp", "list")),
            P(("dp", "list")),
            P(),
            P("list", None),
        ),
        out_specs=(P(("dp", "list"), None), P("list", None)),
        check_vma=False,
    )
```

```python
from functools import partial

import jax
import jax.numpy as jnp
from jax import lax
from jax.experimental import pallas as pl
from jax.experimental.pallas import tpu as pltpu
from jax.sharding import PartitionSpec as P

FINE = 64
LANES = 128
KEY_ROWS = 8
HIGH = 4
MIB = 1024 * 1024
WHOLE = pl.BlockSpec(memory_space=pltpu.VMEM)
SCALAR = pl.BlockSpec(memory_space=pltpu.SMEM)
OUTSIDE = pl.BlockSpec(memory_space=pltpu.HBM)


def iota(shape, dim):
    return lax.broadcasted_iota(jnp.int32, shape, dim)


def ones_where(mask):
    return jnp.where(mask, 1.0, 0.0).astype(jnp.bfloat16)


def product(a, b, dims=((1,), (0,))):
    return lax.dot_general(a, b, (dims, ((), ())), preferred_element_type=jnp.float32)


def one_row(ref):
    return jnp.concatenate([ref[q : q + 1, :] for q in range(ref.shape[0])], axis=1)


def pack_kernel(cap, home_slots, owners, slices, lists_here, coarse_ref, fine_ref, home_ref, rows_ref, out_ref, placed_ref, keys_ref, sent_ref, sems):
    rows = rows_ref.shape[0]
    block = cap + KEY_ROWS
    peers = owners * slices
    coarse, fine = one_row(coarse_ref), one_row(fine_ref)
    table_rows = home_ref.shape[0]
    home = home_ref[...]
    column = ones_where(iota((LANES, rows), 0) == (coarse & (LANES - 1)))
    high = product((home >> 7).astype(jnp.float32).astype(jnp.bfloat16), column)
    low = product((home & 127).astype(jnp.float32).astype(jnp.bfloat16), column)
    in_row = iota((table_rows, rows), 0) == (coarse >> 7)
    position = jnp.sum(jnp.where(in_row, high * 128.0 + low, 0.0), axis=0, keepdims=True).astype(jnp.int32)
    owner = position // lists_here
    slot = position - owner * lists_here
    key = slot * FINE + fine
    group = fine // (FINE // slices)
    target = iota((peers, rows), 0) == owner * slices + group
    mine = iota((owners, rows), 0) == owner
    earlier = ones_where(iota((rows, rows), 0) < iota((rows, rows), 1))
    within = product(ones_where(target), earlier)
    within = jnp.sum(jnp.where(target, within, 0.0), axis=0, keepdims=True).astype(jnp.int32)
    beyond = within >= home_slots
    further = product(ones_where(mine & beyond), earlier)
    further = jnp.sum(jnp.where(mine, further, 0.0), axis=0, keepdims=True).astype(jnp.int32)
    rank = jnp.where(beyond, slices * home_slots + further, group * home_slots + within)
    fits = rank < cap
    over = jnp.max(jnp.where(fits, 0.0, 1.0))
    placed_ref[...] = jnp.where(fits, owner * cap + rank, -1)
    spread = ones_where(iota((LANES, rows), 0) == jnp.where(fits, rank, -1))
    key_high = jnp.where(mine, ((key >> 8) + 1).astype(jnp.float32), 0.0).astype(jnp.bfloat16)
    key_low = jnp.where(mine, (key & 255).astype(jnp.float32), 0.0).astype(jnp.bfloat16)
    lanes_high = product(key_high, spread, ((1,), (1,)))
    lanes_low = product(key_low, spread, ((1,), (1,)))
    line = iota((KEY_ROWS, LANES), 0)
    keys_ref[...] = jnp.zeros_like(keys_ref)
    for o in range(owners):
        tile = jnp.where(line == 0, lanes_high[o : o + 1, :], jnp.where(line == 1, lanes_low[o : o + 1, :], 0.0))
        keys_ref[o * block + cap : (o + 1) * block, :] = jnp.where(line == 2, over, tile)
    where_to = jnp.where(fits, owner * block + rank, -1)
    place = ones_where(iota((owners * block, rows), 0) == where_to)
    copies = []
    for pair in range(slices // 2):
        both = product(place, rows_ref[:, pair * 2 * LANES : (pair + 1) * 2 * LANES])
        for half in range(2):
            piece = both[:, half * LANES : (half + 1) * LANES] + keys_ref[...]
            sent_ref[2 * pair + half, :, :] = piece.astype(jnp.bfloat16)
        at = pl.ds(2 * pair, 2)
        copies.append(pltpu.make_async_copy(sent_ref.at[at], out_ref.at[at], sems.at[pair]))
        copies[-1].start()
    for copy in copies:
        copy.wait()


def middle_kernel(
    cap,
    sources,
    lists_here,
    fine_here,
    got_ref,
    old_ref,
    out_ref,
    new_ref,
    over_ref,
    aug_ref,
    key_ref,
    span_ref,
    near_ref,
    split_ref,
    total_ref,
    tile_ref,
    sent_ref,
    copy_sem,
    sems,
):
    for s in range(0, sources, 16):
        tile_ref[s * KEY_ROWS : (s + 16) * KEY_ROWS, :] = (
            got_ref[s : s + 16, cap : cap + KEY_ROWS, :].astype(jnp.float32).reshape(16 * KEY_ROWS, LANES)
        )
    high = tile_ref[pl.ds(0, sources, stride=KEY_ROWS), :]
    low = tile_ref[pl.ds(1, sources, stride=KEY_ROWS), :]
    over_ref[0, 0] = jnp.max(tile_ref[pl.ds(2, sources, stride=KEY_ROWS), :])
    raw = jnp.where(high > 0.0, (high - 1.0) * 256.0 + low, -1.0)
    key_ref[...] = raw.T.astype(jnp.int32)

    keys = raw.astype(jnp.int32)
    group = jnp.where(keys >= 0, (keys & (FINE - 1)) // fine_here, -1)
    present = jnp.concatenate(
        [jnp.max(jnp.where(group == g, 1.0, 0.0), axis=0, keepdims=True) for g in range(FINE // fine_here)], axis=0
    )
    chunk_of = ones_where(iota((LANES, LANES), 0) // HIGH == iota((LANES, LANES), 1))
    held = ones_where(product(present.astype(jnp.bfloat16), chunk_of) > 0.0)
    meet = product(held, held, ((0,), (0,)))
    away = iota((LANES, LANES), 0) != iota((LANES, LANES), 1)
    span_ref[...] = jnp.where((meet > 0.0) & away, 1, 0)[0 : span_ref.shape[0], :]
    number = jnp.sum(jnp.where((meet > 0.0) & away, 1, 0), axis=1, keepdims=True)[0 : span_ref.shape[0], :]
    span_ref[...] = jnp.where(iota(span_ref.shape, 1) == LANES - 1, number, span_ref[...])
    copy = pltpu.make_async_copy(span_ref, near_ref, copy_sem)
    copy.start()

    part = 16
    for s in range(0, sources, part):
        wide = got_ref[s : s + part, 0:cap, :].astype(jnp.float32)
        aug_ref[:, s : s + part, 0:LANES] = jnp.transpose(wide, (1, 0, 2)).astype(jnp.bfloat16)
    aug_ref[:, :, LANES : 2 * LANES] = jnp.ones((cap, sources, LANES), jnp.bfloat16)
    lists = iota((lists_here, LANES), 0)

    def list_sum(base):
        parts = [ones_where(lists == (key_ref[base + q : base + q + 1, :] >> 6)) for q in range(8)]
        return product(jnp.concatenate(parts, axis=1), aug_ref[base : base + 8].reshape(8 * sources, 2 * LANES))

    sums = sum(list_sum(t) for t in range(0, cap, 8))
    new = (old_ref[...].astype(jnp.float32) + sums[:, 0:LANES]) / (1.0 + sums[:, LANES : 2 * LANES])
    rounded = new.astype(jnp.bfloat16)
    new_ref[...] = rounded
    split_ref[:, 0:LANES] = rounded
    split_ref[:, LANES : 2 * LANES] = (new - rounded.astype(jnp.float32)).astype(jnp.bfloat16)
    copy.wait()

    block = HIGH * sources
    chunks = cap // HIGH

    def columns_of(b):
        own = key_ref[pl.ds(b * HIGH, HIGH), :]
        square = jnp.concatenate([own, jnp.full((LANES - HIGH, LANES), -2, jnp.int32)], axis=0)
        turned = square.astype(jnp.float32).T.astype(jnp.int32)
        return jnp.concatenate([jnp.broadcast_to(turned[:, q : q + 1], (LANES, LANES)) for q in range(HIGH)], axis=0)

    def equal_sum(left, c):
        narrow = left.astype(jnp.int16).reshape(block // 16, 16, LANES)
        parts = []
        for q in range(HIGH):
            row = jnp.broadcast_to(key_ref[pl.ds(c * HIGH + q, 1), :], (16, LANES)).astype(jnp.int16).reshape(1, 16, LANES)
            parts.append(jnp.where(narrow == row, jnp.bfloat16(1), jnp.bfloat16(0)).reshape(block, LANES))
        right = aug_ref[pl.ds(c * HIGH, HIGH)].reshape(block, 2 * LANES)
        return product(jnp.concatenate(parts, axis=1), right)

    def at_block(b):
        return pl.ds(pl.multiple_of(b * block, block), block)

    def diagonal(b):
        left = columns_of(b)
        slots = left >> 6
        parts = [ones_where(slots == iota((block, LANES), 1) + q * LANES) for q in range(lists_here // LANES)]
        centre = product(jnp.concatenate(parts, axis=1), split_ref[...])
        own = equal_sum(left, b)
        total_ref[at_block(b), 0:LANES] = own[:, 0:LANES] + centre[:, 0:LANES] + centre[:, LANES : 2 * LANES]
        total_ref[at_block(b), LANES : 2 * LANES] = own[:, LANES : 2 * LANES] + 1.0

    def both(pair, carry):
        diagonal(2 * pair)
        diagonal(2 * pair + 1)
        return carry

    lax.fori_loop(0, chunks // 2, both, 0)

    def others_of(b, carry):
        @pl.when(near_ref[b, LANES - 1] > 0)
        def _():
            def one(c, inner):
                @pl.when(near_ref[b, c] > 0)
                def _():
                    total_ref[at_block(b), :] += equal_sum(columns_of(b), c)

                return inner

            lax.fori_loop(0, chunks, one, 0)

        return carry

    lax.fori_loop(0, chunks, others_of, 0)
    copies = []
    for s in range(0, sources, part):
        pieces = []
        for k in range(cap):
            at = slice(k * sources + s, k * sources + s + part)
            mean = total_ref[at, 0:LANES] / total_ref[at, LANES : 2 * LANES]
            own = aug_ref[k, s : s + part, 0:LANES].astype(jnp.float32)
            pieces.append((own - mean).reshape(1, part, LANES))
        sent_ref[s : s + part] = jnp.transpose(jnp.concatenate(pieces, axis=0), (1, 0, 2)).astype(jnp.bfloat16)
        at = pl.ds(s, part)
        copies.append(pltpu.make_async_copy(sent_ref.at[at], out_ref.at[at], sems.at[s // part]))
        copies[-1].start()
    for copy in copies:
        copy.wait()


def take_kernel(cap, owners, placed_ref, take_ref):
    rows = take_ref.shape[0]
    placed = placed_ref[...].astype(jnp.float32)
    lines = [placed[:, q * LANES : (q + 1) * LANES] for q in range(rows // LANES)]
    column = jnp.concatenate([jnp.broadcast_to(line, (LANES, LANES)).T for line in lines], axis=0).astype(jnp.int32)
    for r in range(owners * cap // LANES):
        take_ref[:, r * LANES : (r + 1) * LANES] = ones_where(column == iota((rows, LANES), 1) + r * LANES)


def unpack_kernel(cap, owners, slices, mine_ref, take_ref, back_ref, *refs):
    part_refs, (out_ref, new_ref, wide_ref, sent_ref, sems) = refs[:-5], refs[-5:]
    copies = []
    for k, part_ref in enumerate(part_refs):
        wide_ref[k] = part_ref[...].astype(jnp.float32)
        at = pl.multiple_of((mine_ref[0] ^ k) * LANES, LANES)
        copies.append(pltpu.make_async_copy(wide_ref.at[k], new_ref.at[:, pl.ds(at, LANES)], sems.at[k]))
        copies[-1].start()
    take = take_ref[...]
    for d in range(0, slices, 2):
        both = jnp.concatenate([back_ref[d], back_ref[d + 1]], axis=1)
        at = pl.ds(d * LANES, 2 * LANES)
        sent_ref[:, at] = product(take, both).astype(jnp.bfloat16)
        copies.append(pltpu.make_async_copy(sent_ref.at[:, at], out_ref.at[:, at], sems.at[slices + d // 2]))
        copies[-1].start()
    for copy in copies:
        copy.wait()


def call(kernel, outs, scratch, in_specs, out_specs, flops, name, mib):
    return pl.pallas_call(
        kernel,
        out_shape=outs,
        in_specs=in_specs,
        out_specs=out_specs,
        scratch_shapes=scratch,
        compiler_params=pltpu.CompilerParams(vmem_limit_bytes=mib * MIB),
        cost_estimate=pl.CostEstimate(flops=flops, bytes_accessed=4 * MIB, transcendentals=0),
        name=name,
    )


def middle_scratch(cap, peers, lists_here):
    blocks = -(-cap // (8 * HIGH)) * 8
    return [
        pltpu.VMEM((cap, peers, 2 * LANES), jnp.bfloat16),
        pltpu.VMEM((LANES, peers), jnp.int32),
        pltpu.VMEM((blocks, LANES), jnp.int32),
        pltpu.SMEM((blocks, LANES), jnp.int32),
        pltpu.VMEM((lists_here, 2 * LANES), jnp.bfloat16),
        pltpu.VMEM((peers * cap, 2 * LANES), jnp.float32),
        pltpu.VMEM((peers * KEY_ROWS, LANES), jnp.float32),
        pltpu.VMEM((peers, cap, LANES), jnp.bfloat16),
        pltpu.SemaphoreType.DMA,
        pltpu.SemaphoreType.DMA((peers // 16,)),
    ]


def iterate(cap, home_slots, mine, coarse, fine, home, embeddings, coarse_old):
    slices, owners = lax.axis_size("dp"), lax.axis_size("list")
    peers = slices * owners
    rows, width = embeddings.shape
    lists_here = coarse_old.shape[0]
    block = cap + KEY_ROWS
    total = peers * cap
    mib = 26 if cap <= 48 else 56
    shape = jax.ShapeDtypeStruct

    packed, placed = call(
        partial(pack_kernel, cap, home_slots, owners, slices, lists_here),
        (shape((slices, owners * block, LANES), jnp.bfloat16), shape((1, rows), jnp.int32)),
        [
            pltpu.VMEM((owners * block, LANES), jnp.float32),
            pltpu.VMEM((slices, owners * block, LANES), jnp.bfloat16),
            pltpu.SemaphoreType.DMA((slices // 2,)),
        ],
        [WHOLE, WHOLE, WHOLE, WHOLE],
        (OUTSIDE, WHOLE),
        4 * rows * owners * block * width,
        "pack",
        mib,
    )(coarse, fine, home, embeddings)
    got = lax.all_to_all(packed.reshape(peers, block, LANES), ("dp", "list"), 0, 0, tiled=True)
    take = call(
        partial(take_kernel, cap, owners),
        shape((rows, owners * cap), jnp.bfloat16),
        [],
        [WHOLE],
        WHOLE,
        1 << 30,
        "take",
        mib,
    )(placed)
    old_part = lax.dynamic_slice_in_dim(coarse_old, mine * LANES, LANES, 1)
    done, new_part, over = call(
        partial(middle_kernel, cap, peers, lists_here, FINE // slices),
        (
            shape((peers, cap, LANES), jnp.bfloat16),
            shape((lists_here, LANES), jnp.bfloat16),
            shape((1, 1), jnp.float32),
        ),
        middle_scratch(cap, peers, lists_here),
        [WHOLE, WHOLE],
        (OUTSIDE, WHOLE, SCALAR),
        4 * total * (total + lists_here) * LANES,
        "middle",
        mib,
    )(got, old_part)
    pieces = {0: new_part}
    for k in range(2, slices, 2):
        pieces[k] = lax.ppermute(new_part, "dp", [(i, i ^ k) for i in range(slices)])
    for k in range(0, slices, 2):
        pieces[k + 1] = lax.ppermute(pieces[k], "dp", [(i, i ^ 1) for i in range(slices)])
    back = lax.all_to_all(done, ("dp", "list"), 0, 0, tiled=True)

    def finish(mine, take, back, *parts):
        return call(
            partial(unpack_kernel, cap, owners, slices),
            (shape((rows, width), jnp.bfloat16), shape((lists_here, width), jnp.float32)),
            [
                pltpu.VMEM((slices, lists_here, LANES), jnp.float32),
                pltpu.VMEM((rows, width), jnp.bfloat16),
                pltpu.SemaphoreType.DMA((slices + slices // 2,)),
            ],
            [SCALAR] + [WHOLE] * (2 + slices),
            (OUTSIDE, OUTSIDE),
            2 * rows * owners * cap * width,
            "unpack",
            mib,
        )(mine.reshape(1), take, back.reshape(slices, owners * cap, LANES), *parts)

    return over, finish, (mine, take, back) + tuple(pieces[k] for k in range(slices))


def on_device(embeddings, coarse_id, fine_id, list_home, coarse_old):
    rows = embeddings.shape[0]
    args = (
        lax.axis_index("dp"),
        coarse_id.reshape(rows // LANES, LANES),
        fine_id.reshape(rows // LANES, LANES),
        list_home.reshape(-1, LANES),
        embeddings,
        coarse_old,
    )
    over, finish, parts = iterate(40, 4, *args)

    def again(parts, args):
        _, finish_all, parts_all = iterate(96, 12, *args)
        return finish_all(*parts_all)

    return lax.cond(over[0, 0] > 0.0, again, lambda parts, args: finish(*parts), parts, args)


def solution(mesh):
    return jax.shard_map(
        on_device,
        mesh=mesh,
        in_specs=(
            P(("dp", "list"), None),
            P(("dp", "list")),
            P(("dp", "list")),
            P(),
            P("list", None),
        ),
        out_specs=(P(("dp", "list"), None), P("list", None)),
        check_vma=False,
    )
```
